256 devices in a mesh: rep: 2 (over core), dp: 128 (over x, y, z).
Axes of the slice: x: 4, y: 4, z: 8, core: 2. Of those that a mesh axis runs over, the one named last changes fastest.
Arguments:
- g_w_gate: bfloat16 [256, 2, 896, 2560], P(('rep', 'dp')), parts along dimension 0
- g_w_up: bfloat16 [256, 2, 896, 2560], P(('rep', 'dp')), parts along dimension 0
- g_w_down: bfloat16 [256, 2, 2560, 896], P(('rep', 'dp')), parts along dimension 0
- w_gate: bfloat16 [2, 896, 2560], replicated
- w_up: bfloat16 [2, 896, 2560], replicated
- w_down: bfloat16 [2, 2560, 896], replicated
- m_w_gate: float32 [2, 896, 2560], P(None, 'dp')
- m_w_up: float32 [2, 896, 2560], P(None, 'dp')
- m_w_down: float32 [2, 2560, 896], P(None, 'dp')
- v_w_gate: float32 [2, 896, 2560], P(None, 'dp')
- v_w_up: float32 [2, 896, 2560], P(None, 'dp')
- v_w_down: float32 [2, 2560, 896], P(None, 'dp')
Outputs:
- output 1: bfloat16 [4, 896, 2560], P('rep'), parts along dimension 0
- output 2: bfloat16 [4, 896, 2560], P('rep'), parts along dimension 0
- output 3: bfloat16 [4, 2560, 896], P('rep'), parts along dimension 0
- output 4: float32 [4, 896, 2560], P('rep', 'dp'), parts along dimension 0
- output 5: float32 [4, 896, 2560], P('rep', 'dp'), parts along dimension 0
- output 6: float32 [4, 2560, 896], P('rep', 'dp'), parts along dimension 0
- output 7: float32 [4, 896, 2560], P('rep', 'dp'), parts along dimension 0
- output 8: float32 [4, 896, 2560], P('rep', 'dp'), parts along dimension 0
- output 9: float32 [4, 2560, 896], P('rep', 'dp'), parts along dimension 0
There are 2 independent parts. The reference program is written for one: setup_inputs(seed, part) draws one part's arguments, and reference() takes and returns one part's arrays. A program takes and returns all parts, laid end to end along the dimension named above; an argument that names none is the same for every part.
All inputs are finite; a program needn't handle non-finite values.
Results may differ from the reference program's by a relative error of at most 0.022.
Values are sent between devices in bfloat16 or wider.
A program may use at most 768 MiB of HBM per device.

```python
import jax
import jax.numpy as jnp
from jax import lax

DEVICES = 128
D = 896
FF = 2560
LAYERS = 2
NAMES = ("w_gate", "w_up", "w_down")
SHAPES = {"w_gate": (LAYERS, D, FF), "w_up": (LAYERS, D, FF), "w_down": (LAYERS, FF, D)}


def setup_inputs(seed: int = 0, part: int = 0) -> dict:
    kz, *keys = jax.random.split(jax.random.key(seed), 1 + 5 * len(NAMES))
    loud = 2.0 ** jax.random.uniform(kz, (), jnp.float32, -1.0, 1.0)
    drawn = {}
    for name, key, both in zip(NAMES, keys[:3], keys[3:6], strict=True):
        own = jax.random.normal(jax.random.fold_in(key, part), (DEVICES, *SHAPES[name]), jnp.float32)
        shared = jax.random.normal(jax.random.fold_in(both, part), SHAPES[name], jnp.float32)
        drawn["g_" + name] = (loud * (0.7 * shared / DEVICES + 0.7 * own * DEVICES**-0.5)).astype(jnp.bfloat16)
    for name, key in zip(NAMES, keys[6:9], strict=True):
        drawn[name] = (jax.random.normal(key, SHAPES[name], jnp.float32) * SHAPES[name][1] ** -0.5).astype(jnp.bfloat16)
    for name, key in zip(NAMES, keys[9:12], strict=True):
        drawn["m_" + name] = loud * 0.5 * jax.random.normal(key, SHAPES[name], jnp.float32)
    for name, key in zip(NAMES, keys[12:15], strict=True):
        drawn["v_" + name] = loud * loud * jax.random.uniform(key, SHAPES[name], jnp.float32, 0.5, 1.5)
    return drawn


def adamw(w, m, v, g):
    m = 0.9 * m + 0.1 * g
    v = 0.95 * v + 0.05 * g * g
    step = m * lax.rsqrt(v + 1e-8) + 0.1 * w
    return (w - 0.02 * step).astype(jnp.bfloat16), m, v


def clipped(gradients, sum_of_squares, count):
    factor = jnp.minimum(1.0, 0.5 * lax.rsqrt(sum_of_squares / count + 1e-30))
    return [g * factor for g in gradients]


def reference(g_w_gate, g_w_up, g_w_down, w_gate, w_up, w_down, m_w_gate, m_w_up, m_w_down, v_w_gate, v_w_up, v_w_down):
    def total(terms):
        return lax.scan(lambda so_far, term: (so_far + term.astype(jnp.float32), None), jnp.zeros(terms.shape[1:], jnp.float32), terms)[0]

    gradients = [total(terms).astype(jnp.bfloat16).astype(jnp.float32) for terms in (g_w_gate, g_w_up, g_w_down)]
    gradients = clipped(gradients, sum(jnp.sum(g * g) for g in gradients), sum(g.size for g in gradients))
    new = [
        adamw(w.astype(jnp.float32), m, v, g)
        for w, m, v, g in zip((w_gate, w_up, w_down), (m_w_gate, m_w_up, m_w_down), (v_w_gate, v_w_up, v_w_down), gradients, strict=True)
    ]
    return tuple(one[which] for which in range(3) for one in new)
```

```python
import jax
import jax.numpy as jnp
from jax import lax
from jax.experimental import pallas as pl
from jax.experimental.pallas import tpu as pltpu
from jax.sharding import PartitionSpec as P

MESH = pl.DeviceIdType.MESH
F32, BF16 = jnp.float32, jnp.bfloat16
X, Y, Z = 4, 4, 8
SIZE = {"x": X, "y": Y, "z": Z}
DIMS = {"A": ("x", "y", "z"), "B": ("y", "z", "x"), "C": ("z", "x", "y")}
COLOURS = tuple(DIMS)
LAYERS, ROWS, LANES = 2, 8, 128
TILE = (ROWS, LANES)
D, FF = 896, 2560
HIGH, HALF, LEFT, PART = 7, 10, 6, 5
BLOCK = {"A": (HIGH, LEFT), "B": (PART, HIGH), "C": (HIGH, HALF - LEFT)}
COUNT = 3 * LAYERS * D * FF


def lens(c):
    return tuple(SIZE[d] for d in DIMS[c])


def tiles(c):
    return BLOCK[c][0] * BLOCK[c][1]


def down_place(z):
    return (0, (z + 1) // 2 % X) if z % 2 else (1, (z // 2 + 3) % X)


def ring(n, ant):
    return [(ant, n // 2)] + [(d, k) for k in range(n // 2 - 1, 0, -1) for d in (1, -1)]


def slots(n, ant):
    return {m: i for i, m in enumerate(sorted(ring(n, ant), key=lambda m: (m[1], -m[0])))}


def far_first(n):
    return [n // 2] + [s * k for k in range(n // 2 - 1, 0, -1) for s in (1, -1)] + [0]


def ant_of(o):
    return -1 if o % 2 else 1


def ant_in(phase, unit):
    return (1, ant_of(sum(o for o in unit if o is not None)) if unit else 1)[phase < 3]


def came(c, phase, unit, n, o):
    far = n - o < n // 2 or (n == 2 * o and ant_in(phase, unit) == 1)
    return (c, phase, unit, 1, n - o) if far else (c, phase, unit, -1, o)


def gather_messages():
    out = {}
    for c in COLOURS:
        n1, n2, n3 = lens(c)

        def add(phase, unit, count, first):
            dim = DIMS[c][phase - 1]
            for d, k in ring(SIZE[dim], ant_in(phase, unit)):
                out[c, phase, unit, d, k] = ((dim, d), count * tiles(c), [(c, phase, unit, d, k - 1)] if k > 1 else first)

        add(3, (), 1, [])
        for o in range(n3):
            first = [came(c, 3, (), n3, o)] if o else []
            add(2, (o,), 1, first)
            add(1, (0, o), 1, first)
        for o in range(1, n2):
            add(1, (o, None), n3, [came(c, 2, (i,), n2, o) for i in range(n3)])
    return out


def ordered(messages, slack, latency, rate):
    users, tail = {t: [] for t in messages}, {}
    for t, (_, _, waits) in messages.items():
        for w in waits:
            users[w].append(t)

    def way(t):
        if t not in tail:
            tail[t] = 2 * messages[t][1] / rate + latency + max((way(u) for u in users[t]), default=0)
        return tail[t]

    for t in messages:
        way(t)
    queues = {m[0]: [] for m in messages.values()}
    left, arrives, now, starts = list(messages), {}, 0.0, []
    while left or any(queues.values()):
        ready = [
            t
            for t in left
            if all(arrives.get(w, now + 1) <= now for w in messages[t][2]) and 2 * sum(q[1] for q in queues[messages[t][0]]) <= slack
        ]
        if ready:
            t = max(ready, key=way)
            left.remove(t)
            starts.append(t)
            queues[messages[t][0]].append([t, messages[t][1] / rate])
            continue
        speed = {(m, d): 1 / 2 if queues[m, -d] else 1 for (m, d), q in queues.items() if q}
        full = {link: sum(q[1] for q in queues[link]) - slack / 2 for link in speed}
        events = [queues[link][0][1] / s for link, s in speed.items()] + [full[link] / s for link, s in speed.items() if full[link] > 0]
        pause = min(events + [a - now for a in arrives.values() if a > now]) + 1e-6
        now += pause
        for link, s in speed.items():
            queues[link][0][1] -= pause * s
            if queues[link][0][1] <= 0:
                arrives[queues[link].pop(0)[0]] = now + latency
    return starts, list(arrives), arrives


GATHER = gather_messages()
GATHER_ORDER, ENDS, GATHER_AT = ordered(GATHER, 2.0, 2.0, 43.0)


def back(t):
    c, phase, unit, d, k = t
    return (c, phase, unit, -d, k)


REDUCE = {back(t): (link, n, []) for t, (link, n, _) in GATHER.items()}
for t, (_, _, waits) in GATHER.items():
    for w in waits:
        REDUCE[back(w)][2].append(back(t))
REDUCE_ORDER = [back(t) for t in reversed(ENDS)]
R_ID = {t: i for i, t in enumerate(REDUCE)}
G_ID = {t: i for i, t in enumerate(GATHER)}


class Place:
    def __init__(self):
        dp = lax.axis_index("dp")
        rep = lax.axis_index("rep")
        self.at = at = {"x": lax.div(dp, Y * Z), "y": lax.rem(lax.div(dp, Z), Y), "z": lax.rem(dp, Z)}
        sign = 1 - 2 * rep
        self.offset = {(d, k): lax.rem(at[d] + sign * k + n, n) for d, n in SIZE.items() for k in range(-n // 2, n // 2) if k}

        def device(**moved):
            a = {**at, **moved}
            return (rep, (a["x"] * Y + a["y"]) * Z + a["z"])

        def ahead(d, k):
            return lax.rem(at[d] + SIZE[d] + k, SIZE[d])

        self.device = device
        self.beside = {(d, e): device(**{d: self.offset[d, e]}) for d in SIZE for e in (1, -1)}
        self.line = [ahead("z", k) for k in range(Z)]
        self.line_from = [ahead("z", -k) for k in range(Z)]
        self.line_device = [device(z=to) for to in self.line]
        self.plane_device = [device(x=ahead("x", k // Y), y=ahead("y", k % Y)) for k in range(X * Y)]
        self.plane_from = [Y * ahead("x", -(k // Y)) + ahead("y", -(k % Y)) for k in range(X * Y)]

    def off(self, dim, k):
        n = SIZE[dim]
        k = (k + n // 2) % n - n // 2
        return self.offset[dim, k] if k else self.at[dim]


def fence(p):
    peers = p.line_device[1:] + p.plane_device[1:]
    barrier = pltpu.get_barrier_semaphore()
    for peer in peers:
        pl.semaphore_signal(barrier, inc=1, device_id=peer, device_id_type=MESH)
    pl.semaphore_wait(barrier, len(peers))


def start_loads(p, gate, up, down, T, sem):
    for step in range(Z):
        for c in COLOURS:
            n1 = lens(c)[0]
            if step >= n1:
                continue
            k = far_first(n1)[step]
            j = p.off(DIMS[c][0], k)
            s = sem[c].at[k % n1]
            if c == "A":
                for z in range(Z):
                    src = (gate, up)[z // X].at[z // 2 % 2, j, :, :, z % 2, pl.ds(0, LEFT)]
                    pltpu.make_async_copy(src, T[c].at[j, :, z], s).start()
            elif c == "B":
                for z in range(Z):
                    layer, q = down_place(z)
                    pltpu.make_async_copy(down.at[layer, :, j, q], T[c].at[j, z], s).start()
            else:
                layer, half = lax.rem(lax.div(j, 2), 2), lax.rem(j, 2)

                def load(ref):
                    pltpu.make_async_copy(ref.at[layer, :, :, :, half, pl.ds(LEFT, HALF - LEFT)], T[c].at[j], s).start()

                pl.when(j < X)(lambda: load(gate))
                pl.when(j >= X)(lambda: load(up))


class Reduce:
    def __init__(self, p, T, O, load, sent, arrived):
        self.p, self.T, self.O, self.load, self.sent, self.arrived = p, T, O, load, sent, arrived
        self.waited, self.loaded = set(), set()

    def areas(self, t):
        c, phase, unit, d, k = t
        n1, n2, n3 = lens(c)
        d1, d2, d3 = DIMS[c]
        p = self.p
        slot = slots(SIZE[DIMS[c][phase - 1]], -ant_in(phase, unit))[d, k]
        if phase == 1:
            j2 = p.off(d2, unit[0])
            first, count = (0, n3) if unit[1] is None else (p.off(d3, unit[1]), 1)
            return (p.off(d1, d * k), j2), first, (slot, j2), first, count
        if phase == 2:
            j3 = p.off(d3, unit[0])
            return (p.at[d1], p.off(d2, d * k)), j3, (n1 - 1, slot), j3, 1
        return (p.at[d1], p.at[d2]), p.off(d3, d * k), (n1 - 1, n2 - 1), slot, 1

    def copy(self, t):
        c, phase, _, d, _ = t
        src, i, dst, j, n = self.areas(t)
        s = R_ID[t]
        return pltpu.make_async_remote_copy(
            src_ref=self.T[c].at[(*src, pl.ds(i, n))],
            dst_ref=self.O[c].at[(*dst, pl.ds(j, n))],
            send_sem=self.sent.at[s],
            recv_sem=self.arrived.at[s],
            device_id=self.p.beside[DIMS[c][phase - 1], d],
            device_id_type=MESH,
        )

    def wait(self, t):
        if t not in self.waited:
            self.waited.add(t)
            self.copy(t).wait_recv()

    def wait_load(self, c, k):
        k %= lens(c)[0]
        if (c, k) not in self.loaded:
            self.loaded.add((c, k))
            ref = self.T[c].at[self.p.off(DIMS[c][0], k)]
            pltpu.make_async_copy(ref, ref, self.load[c].at[k]).wait()

    def ended(self, c, phase, j2, j3):
        last = lens(c)[0] - 1
        return [(0, j2, j3), (1, j2, j3), (last, 0, j3), (last, 1, j3)][: 2 * (phase - 1)]

    def send(self, t):
        c, phase, unit, d, k = t
        T, O = self.T[c], self.O[c]
        for w in REDUCE[t][2]:
            self.wait(w)
        self.wait_load(c, d * k if phase == 1 else 0)
        src, first, _, _, count = self.areas(t)
        before = (c, phase, unit, d, k + 1)
        chain = before in R_ID
        if phase > 1 or chain:
            _, _, there, start, _ = self.areas(before if chain else t)

            def one(i):
                parts = self.ended(c, phase, src[1], first + i)
                if chain:
                    parts.append((*there, start + i))
                total = T[(*src, first + i)].astype(F32)
                for part in parts:
                    total = total + O[part].astype(F32)
                T[(*src, first + i)] = total.astype(BF16)

            if count == 1:
                one(0)
            else:
                pl.loop(0, count)(one)
        self.copy(t).start()

    def own(self, c):
        n1, n2, _ = lens(c)
        for t in REDUCE:
            if t[0] == c and t[-1] == 1 and t[2] in ((), (0,), (0, 0)):
                self.wait(t)
        self.wait_load(c, 0)
        i, j, k = (self.p.at[d] for d in DIMS[c])
        total = self.T[c][i, j, k].astype(F32)
        for part in self.ended(c, 3, j, k) + [(n1 - 1, n2 - 1, e) for e in (0, 1)]:
            total = total + self.O[c][part].astype(F32)
        return total.astype(BF16).astype(F32)


class Gather:
    def __init__(self, p, O, sent, arrived):
        self.p, self.O, self.sent, self.arrived = p, O, sent, arrived
        self.waited = set()

    def copy(self, t, came=0):
        c, phase, unit, d, k = t
        d1, d2, d3 = DIMS[c]
        p, dim = self.p, DIMS[c][phase - 1]
        behind = p.off(dim, d * (1 - came - k))
        if phase == 1:
            at = (behind, p.off(d2, unit[0])) if unit[1] is None else (behind, p.off(d2, unit[0]), p.off(d3, unit[1]))
        else:
            at = (p.at[d1], behind, p.off(d3, unit[0])) if phase == 2 else (p.at[d1], p.at[d2], behind)
        ref, s = self.O[c].at[at], G_ID[t]
        return pltpu.make_async_remote_copy(
            src_ref=ref, dst_ref=ref, send_sem=self.sent.at[s], recv_sem=self.arrived.at[s], device_id=p.beside[dim, d], device_id_type=MESH
        )

    def wait(self, t):
        if t not in self.waited:
            self.waited.add(t)
            self.copy(t, 1).wait_recv()

    def send(self, t):
        for w in GATHER[t][2]:
            self.wait(w)
        self.copy(t).start()


def rows_of(a):
    return lax.broadcasted_iota(jnp.int32, a.shape, a.ndim - 2)


def joined(a, b, k):
    return pltpu.roll(jnp.where(rows_of(b) >= ROWS - k, a, b), k, b.ndim - 2)


def adamw(w, m, v, g):
    m = 0.9 * m + 0.1 * g
    v = 0.95 * v + 0.05 * g * g
    return w - 0.02 * (m * lax.rsqrt(v + 1e-8) + 0.1 * w), m, v


DOWN_ROWS = (ROWS, ROWS, ROWS // 2)
SCRATCH = {
    "raw": ((2, 2, HIGH, LAYERS, FF), F32),
    "raw_down": ((2, 20, LAYERS, D), F32),
    "old": ((2, LAYERS, 2, 2, HALF, *TILE), BF16),
    "old_down": ((LAYERS, 3, HIGH, *TILE), BF16),
    "w": ((2, LAYERS, 2 * HALF, *TILE), F32),
    "w_low": ((LAYERS, 3, HIGH, *TILE), F32),
    "mv": ((2, 2, LAYERS, 2 * HALF, *TILE), F32),
    "mv_low": ((2, LAYERS, 3, HIGH, *TILE), F32),
    "out": ((Z, HALF, *TILE), BF16),
    "into": ((Z, HALF, *TILE), BF16),
    "out_low": ((2, 3, HIGH, *TILE), BF16),
    "into_low": ((LAYERS, 3, HIGH, *TILE), BF16),
    "new": ((Z, HALF, *TILE), BF16),
    "news": ((Z, HALF, *TILE), BF16),
    "new_low": ((LAYERS, 3, HIGH, *TILE), BF16),
    "news_low": ((2, 3, HIGH, *TILE), BF16),
    "z_sum": ((Z, *TILE), F32),
    "sum": ((X * Y, *TILE), F32),
}


class Few:
    def __init__(self, p, sent, arrived):
        self.p, self.sent, self.arrived, self.pushed, self.used = p, sent, arrived, [], 0

    def places(self, n):
        self.used += n
        return self.used - n

    def push(self, src, dst, i, j, to):
        one = pltpu.make_async_remote_copy(
            src_ref=src, dst_ref=dst, send_sem=self.sent.at[i], recv_sem=self.arrived.at[j], device_id=to, device_id_type=MESH
        )
        self.pushed.append(one)
        one.start()

    def arrive(self, ref, i):
        pltpu.make_async_copy(ref, ref, self.arrived.at[i]).wait()

    def line(self, out, into):
        p, base = self.p, self.places(Z)
        z = p.at["z"]
        for k in range(1, Z):
            self.push(out.at[p.line[k]], into.at[z], base + k, base + k, p.line_device[k])

        def wait():
            for k in range(1, Z):
                self.arrive(into.at[p.line_from[k]], base + k)

        return wait


def lanes(c):
    return pl.ds(pl.multiple_of(c * LANES, LANES), LANES)


def work(*refs):
    terms, weights, moments, refs = refs[:3], refs[3:6], refs[6:12], refs[12:]
    outs, made, refs = refs[:3], refs[3:9], refs[9:]
    O, T, refs = dict(zip(COLOURS, outs)), dict(zip(COLOURS, refs)), refs[3:]
    s = dict(zip(SCRATCH, refs))
    *load, small, r_sent, r_arrived, g_sent, g_arrived, x_sent, x_arrived = refs[len(SCRATCH) :]
    p = Place()
    x, y, z = p.at.values()
    start_loads(p, *terms, T, dict(zip(COLOURS, load)))

    plain = []

    def fetch(src, dst):
        plain.append(pltpu.make_async_copy(src, dst, small.at[len(plain)]))
        plain[-1].start()

    first = (X * Y * PART) * x + 20 * y + lax.div(PART * z, 2)
    for layer in range(LAYERS):
        for w in range(2):
            for i, row in enumerate((lax.max(z - 1, 0), lax.min(z, HIGH - 1))):
                fetch(weights[w].at[layer, x, y, row], s["old"].at[w, layer, i])
        fetch(weights[2].at[layer, pl.ds(first, 3)], s["old_down"].at[layer])
    for i in range(2):
        for w in range(2):
            fetch(moments[3 * i + w], s["raw"].at[i, w])
        fetch(moments[3 * i + 2], s["raw_down"].at[i])

    def unpack():
        for one in plain:
            one.wait()
        for layer in range(LAYERS):
            for w in range(2):
                low, high = (s["old"][w, layer, i].reshape(2 * HALF, *TILE).astype(F32) for i in range(2))
                s["w"][w, layer] = joined(low, high, z)
            part = [s["old_down"][layer, j].astype(F32) for j in range(3)]
            for j in range(3):
                s["w_low"][layer, j] = jnp.where(lax.rem(z, 2) == 1, joined(part[j], part[min(j + 1, 2)], ROWS // 2), part[j])

        @pl.loop(0, 2 * HALF)
        def _(c):
            for i in range(2):
                for w in range(2):
                    for layer in range(LAYERS):
                        s["mv"][i, w, layer, c, pl.ds(0, HIGH)] = s["raw"][i, w, :, layer, lanes(c)]

        @pl.loop(0, HIGH)
        def _(c):
            for i in range(2):
                for layer in range(LAYERS):
                    for j, n in enumerate(DOWN_ROWS):
                        s["mv_low"][i, layer, j, c, pl.ds(0, n)] = s["raw_down"][i, pl.ds(ROWS * j, n), layer, lanes(c)]

    fence(p)
    reduce = Reduce(p, T, O, dict(zip(COLOURS, load)), r_sent, r_arrived)
    for n, t in enumerate(REDUCE_ORDER):
        if 2 * n == len(REDUCE_ORDER):
            unpack()
        reduce.send(t)

    few = Few(p, x_sent, x_arrived)
    squares = jnp.zeros(TILE, F32)
    for c in ("C", "A"):
        g = reduce.own(c)
        n = BLOCK[c][1]
        place = pl.ds(0 if c == "A" else LEFT, n)
        squares = squares + jnp.sum((g * g).reshape(HIGH * n, *TILE), axis=0)
        for k in range(Z):
            before, at = g[max(k - 1, 0)], g[min(k, HIGH - 1)]
            s["out"][k, place] = (joined(before, at, k) if k else at).astype(BF16)
    pieces = few.line(s["out"], s["into"])
    s["into"][z] = s["out"][z]

    g = reduce.own("B")
    squares = squares + jnp.sum((g * g).reshape(PART * HIGH, *TILE), axis=0)
    for j in range(3):
        s["out_low"][0, j] = g[j].astype(BF16)
        s["out_low"][1, j] = joined(g[2 + j], g[min(3 + j, PART - 1)], ROWS // 2).astype(BF16)
    my_layer = 1 - lax.rem(z, 2)
    my_pair = lax.rem(lax.div(z + 1, 2) + 3 * my_layer, X)
    low = few.places(2)
    for i in range(2):
        few.push(s["out_low"].at[i], s["into_low"].at[my_layer], low + i, low + my_layer, p.device(z=2 * my_pair + i))

    base = few.places(Z)
    s["z_sum"][z] = squares
    for k in range(1, Z):
        few.push(s["z_sum"].at[z], s["z_sum"].at[z], base + k, base + k, p.line_device[k])
    for k in range(1, Z):
        few.arrive(s["z_sum"].at[p.line_from[k]], base + k)
    base, mine = few.places(X * Y), Y * x + y
    s["sum"][mine] = jnp.sum(s["z_sum"][...], axis=0)
    for k in range(1, X * Y):
        few.push(s["sum"].at[mine], s["sum"].at[mine], base + k, base + k, p.plane_device[k])
    pieces()
    for layer in range(LAYERS):
        few.arrive(s["into_low"].at[layer], low + layer)
    for k in range(1, X * Y):
        few.arrive(s["sum"].at[p.plane_from[k]], base + k)
    total = jnp.sum(s["sum"][...], axis=0)
    total = jnp.sum(jnp.sum(total, axis=1, keepdims=True), axis=0, keepdims=True)
    factor = jnp.minimum(1.0, 0.5 * lax.rsqrt(total / COUNT + 1e-30))

    for owner in range(Z):
        w, layer, part = owner // X, owner // 2 % 2, pl.ds(owner % 2 * HALF, HALF)
        g = s["into"][owner].astype(F32) * factor
        new, m, v = adamw(s["w"][w, layer, part], s["mv"][0, w, layer, part], s["mv"][1, w, layer, part], g)
        s["mv"][0, w, layer, part], s["mv"][1, w, layer, part] = m, v
        s["new"][owner] = new.astype(BF16)
    back_pieces = few.line(s["new"], s["news"])
    for layer in range(LAYERS):
        g = s["into_low"][layer].astype(F32) * factor
        new, m, v = adamw(s["w_low"][layer], s["mv_low"][0, layer], s["mv_low"][1, layer], g)
        s["mv_low"][0, layer], s["mv_low"][1, layer] = m, v
        s["new_low"][layer] = new.astype(BF16)
    s["news"][z] = s["new"][z]
    low, parity = few.places(2), lax.rem(z, 2)
    for layer in range(LAYERS):
        to = lax.rem(z - parity + (Z - 1, 2)[layer], Z)
        few.push(s["new_low"].at[layer], s["news_low"].at[parity], low + layer, low + parity, p.device(z=to))

    own = {c: tuple(p.at[d] for d in DIMS[c]) for c in COLOURS}
    back_pieces()
    t = [s["news"][k].astype(F32) for k in range(Z)]
    for i in range(HIGH):
        a = pltpu.roll(t[i], ROWS - i, 1) if i else t[i]
        tile = jnp.where(rows_of(a) < HIGH - i, a, pltpu.roll(t[i + 1], HIGH - i, 1)).astype(BF16)
        O["A"][(*own["A"], i)] = tile[:LEFT]
        O["C"][(*own["C"], i)] = tile[LEFT:]
    for i in range(2):
        few.arrive(s["news_low"].at[i], low + i)
    a, b = ([s["news_low"][i, j].astype(F32) for j in range(3)] for i in range(2))
    seam = jnp.where(rows_of(b[0]) < ROWS // 2, a[2], pltpu.roll(b[0], ROWS // 2, 1))
    for i, tile in enumerate((a[0], a[1], seam, *(joined(b[j], b[j + 1], ROWS // 2) for j in range(2)))):
        O["B"][(*own["B"], i)] = tile.astype(BF16)

    gather = Gather(p, O, g_sent, g_arrived)
    for n, t in enumerate(GATHER_ORDER):
        gather.send(t)
        if 2 * n == len(GATHER_ORDER):

            @pl.loop(0, 2 * HALF)
            def _(c):
                for i in range(2):
                    for w in range(2):
                        for layer in range(LAYERS):
                            rows = pl.ds(LAYERS * c + layer, HIGH, stride=LAYERS * 2 * HALF)
                            made[3 * i + w][rows, :] = s["mv"][i, w, layer, c, pl.ds(0, HIGH)]

            @pl.loop(0, HIGH)
            def _(c):
                for i in range(2):
                    for layer in range(LAYERS):
                        for j, k in enumerate(DOWN_ROWS):
                            rows = pl.ds(ROWS * j * LAYERS * HIGH + LAYERS * c + layer, k, stride=LAYERS * HIGH)
                            made[3 * i + 2][rows, :] = s["mv_low"][i, layer, j, c, pl.ds(0, k)]

            for one in [reduce.copy(t) for t in REDUCE] + few.pushed:
                one.wait_send()
    for t in GATHER_ORDER:
        gather.wait(t)
    for t in GATHER:
        gather.copy(t).wait_send()


def put(*refs):
    (a, b, c), moments, (gate, up, down), results, sem = refs[:3], refs[3:9], refs[9:12], refs[12:18], refs[18]
    pairs = list(zip(moments, results))
    for z in range(Z):
        ref, layer, half = (gate, up)[z // X], z // 2 % 2, z % 2
        pairs.append((a.at[:, :, z], ref.at[layer, :, :, :, half, pl.ds(0, LEFT)]))
        pairs.append((c.at[z], ref.at[layer, :, :, :, half, pl.ds(LEFT, HALF - LEFT)]))
        layer, q = down_place(z)
        pairs += [(b.at[y, z], down.at[layer, :, y, q]) for y in range(Y)]
    copies = [pltpu.make_async_copy(src, dst, sem.at[i]) for i, (src, dst) in enumerate(pairs)]
    for one in copies:
        one.start()
    for one in copies:
        one.wait()


def tiled(a, *cut):
    rows, columns = cut
    n = len(rows)
    a = a.reshape(LAYERS, *rows, ROWS, *columns, LANES)
    order = [*range(n + 1), *range(n + 2, n + 2 + len(columns)), n + 1, a.ndim - 1]
    return a.transpose(order)


def untiled(a, *cut):
    rows, columns = cut
    n = len(rows)
    order = [*range(n + 1), a.ndim - 2, *range(n + 1, a.ndim - 2), a.ndim - 1]
    a = a.transpose(order)
    return a.reshape(LAYERS, -1, a.shape[-1] * (HALF * 2 if len(columns) == 2 else HIGH))


WIDE, TALL = ((X, Y, HIGH), (2, HALF)), ((X, Y, X, PART), (HIGH,))


def unmoment(a, rows, columns):
    return a.reshape(rows, columns, LAYERS, LANES).transpose(0, 2, 1, 3).reshape(rows, LAYERS, columns * LANES).transpose(1, 0, 2)


def solution(mesh):
    shapes = [pltpu.VMEM((*lens(c), *BLOCK[c], *TILE), BF16) for c in COLOURS]
    hbm, vmem = pl.BlockSpec(memory_space=pltpu.HBM), pl.BlockSpec(memory_space=pltpu.VMEM)
    moment = (LAYERS * HIGH * HALF * 2, LANES)

    def semaphores(n):
        return pltpu.SemaphoreType.DMA((n,))

    def kernel(body, name, params, **more):
        return pl.pallas_call(body, name=name, compiler_params=pltpu.CompilerParams(**params), **more)

    def step(*arrays):
        terms, weights, moments = [t[0] for t in arrays[:3]], arrays[3:6], arrays[6:]
        wide = [tiled(a, *WIDE) for a in (*terms[:2], *weights[:2])]
        operands = [*wide[:2], tiled(terms[2], *TALL), *wide[2:], tiled(weights[2], (FF // ROWS,), (HIGH,))]
        operands += [a.transpose(1, 0, 2) for a in moments]
        made = kernel(
            work,
            "work",
            dict(collective_id=0, has_side_effects=True, vmem_limit_bytes=34 << 20),
            out_shape=(*shapes, *[pltpu.VMEM(moment, F32)] * 6),
            in_specs=[hbm] * 12,
            out_specs=[vmem] * 9,
            scratch_shapes=[
                *shapes,
                *(pltpu.VMEM(*a) for a in SCRATCH.values()),
                *(semaphores(lens(c)[0]) for c in COLOURS),
                semaphores(16),
                *(semaphores(n) for n in (len(REDUCE), len(REDUCE), len(GATHER), len(GATHER), 64, 64)),
            ],
        )(*(pltpu.with_memory_space_constraint(a, pltpu.HBM) for a in operands))
        out = kernel(
            put,
            "put",
            dict(vmem_limit_bytes=1 << 20),
            out_shape=[jax.ShapeDtypeStruct(a.shape, BF16) for a in operands[:3]] + [jax.ShapeDtypeStruct(moment, F32)] * 6,
            in_specs=[vmem] * 9,
            out_specs=[hbm] * 9,
            scratch_shapes=[semaphores(54)],
        )(*made)
        weights = [untiled(a, *cut) for a, cut in zip(out, (WIDE, WIDE, TALL))]
        return (*weights, *(unmoment(a, *m.shape[1:2], m.shape[2] // LANES) for a, m in zip(out[3:], moments)))

    all_of, cut = P(None, None, None), P(None, "dp", None)
    return jax.shard_map(
        step,
        mesh=mesh,
        in_specs=(P(("rep", "dp"), None, None, None),) * 3 + (all_of,) * 3 + (cut,) * 6,
        out_specs=(P("rep", None, None),) * 3 + (P("rep", "dp", None),) * 6,
        check_vma=False,
    )
```

```python
import functools

import jax
import jax.numpy as jnp
from jax import lax
from jax.experimental import pallas as pl
from jax.experimental.pallas import tpu as pltpu
from jax.sharding import PartitionSpec as P

MESH = pl.DeviceIdType.MESH
F32, BF16 = jnp.float32, jnp.bfloat16
X, Y, Z = 4, 4, 8
SIZE = {"x": X, "y": Y, "z": Z}
DIMS = {"A": ("x", "y", "z"), "B": ("y", "z", "x"), "C": ("z", "x", "y")}
COLOURS = tuple(DIMS)
LAYERS, ROWS, LANES = 2, 8, 128
TILE = (ROWS, LANES)
D, FF = 896, 2560
HIGH, HALF, LEFT, PART = 7, 10, 6, 5
BLOCK = {"A": (HIGH, LEFT), "B": (PART, HIGH), "C": (HIGH, HALF - LEFT)}
COUNT = 3 * LAYERS * D * FF


def lens(c):
    return tuple(SIZE[d] for d in DIMS[c])


def tiles(c):
    return BLOCK[c][0] * BLOCK[c][1]


def down_place(z):
    return z % 2, z // 2


def ring(n, ant):
    return [(ant, n // 2)] + [(d, k) for k in range(n // 2 - 1, 0, -1) for d in (1, -1)]


def slots(n, ant):
    return {m: i for i, m in enumerate(sorted(ring(n, ant), key=lambda m: (m[1], -m[0])))}


def far_first(n):
    return [n // 2] + [s * k for k in range(n // 2 - 1, 0, -1) for s in (1, -1)] + [0]


def ant_of(o):
    return -1 if o % 2 else 1


def ant_in(phase, unit):
    return (1, ant_of(sum(o for o in unit if o is not None)) if unit else 1)[phase < 3]


def came(c, phase, unit, n, o):
    far = n - o < n // 2 or (n == 2 * o and ant_in(phase, unit) == 1)
    return (c, phase, unit, 1, n - o) if far else (c, phase, unit, -1, o)


def gather_messages():
    out = {}
    for c in COLOURS:
        n1, n2, n3 = lens(c)

        def add(phase, unit, count, first):
            dim = DIMS[c][phase - 1]
            for d, k in ring(SIZE[dim], ant_in(phase, unit)):
                out[c, phase, unit, d, k] = ((dim, d), count * tiles(c), [(c, phase, unit, d, k - 1)] if k > 1 else first)

        add(3, (), 1, [])
        for o in range(n3):
            first = [came(c, 3, (), n3, o)] if o else []
            add(2, (o,), 1, first)
            add(1, (0, o), 1, first)
        for o in range(1, n2):
            add(1, (o, None), n3, [came(c, 2, (i,), n2, o) for i in range(n3)])
    return out


def ordered(messages, slack, latency, rate):
    users, tail = {t: [] for t in messages}, {}
    for t, (_, _, waits) in messages.items():
        for w in waits:
            users[w].append(t)

    def way(t):
        if t not in tail:
            tail[t] = 2 * messages[t][1] / rate + latency + max((way(u) for u in users[t]), default=0)
        return tail[t]

    for t in messages:
        way(t)
    queues = {m[0]: [] for m in messages.values()}
    left, arrives, now, starts = list(messages), {}, 0.0, []
    while left or any(queues.values()):
        ready = [
            t
            for t in left
            if all(arrives.get(w, now + 1) <= now for w in messages[t][2])
            and 2 * sum(q[1] for q in queues[messages[t][0]]) <= slack
        ]
        if ready:
            t = max(ready, key=way)
            left.remove(t)
            starts.append(t)
            queues[messages[t][0]].append([t, messages[t][1] / rate])
            continue
        speed = {(m, d): 1 / 2 if queues[m, -d] else 1 for (m, d), q in queues.items() if q}
        full = {link: sum(q[1] for q in queues[link]) - slack / 2 for link in speed}
        events = [queues[link][0][1] / s for link, s in speed.items()] + [full[link] / s for link, s in speed.items() if full[link] > 0]
        pause = min(events + [a - now for a in arrives.values() if a > now]) + 1e-6
        now += pause
        for link, s in speed.items():
            queues[link][0][1] -= pause * s
            if queues[link][0][1] <= 0:
                arrives[queues[link].pop(0)[0]] = now + latency
    return starts, list(arrives), arrives


GATHER = gather_messages()
GATHER_ORDER, ENDS, GATHER_AT = ordered(GATHER, 2.0, 2.0, 43.0)


def back(t):
    c, phase, unit, d, k = t
    return (c, phase, unit, -d, k)


REDUCE = {back(t): (link, n, []) for t, (link, n, _) in GATHER.items()}
for t, (_, _, waits) in GATHER.items():
    for w in waits:
        REDUCE[back(w)][2].append(back(t))
REDUCE_ORDER = [back(t) for t in reversed(ENDS)]
R_ID = {t: i for i, t in enumerate(REDUCE)}
G_ID = {t: R_ID[back(t)] for t in GATHER}
S_ID = {t: i for i, t in enumerate((c, phase) for c in COLOURS for phase in range(1, 4))}


def all_sent(T, sem):
    for (c, phase), i in S_ID.items():
        n = lens(c)[phase - 1] - 1
        ref = T[c].at[(*[0] * (phase - 1), pl.ds(0, n))]
        pltpu.make_async_copy(ref, ref, sem.at[i]).wait()


class Place:
    def __init__(self):
        dp = lax.axis_index("dp")
        rep = lax.axis_index("rep")
        self.at = at = {"x": lax.div(dp, Y * Z), "y": lax.rem(lax.div(dp, Z), Y), "z": lax.rem(dp, Z)}
        sign = 1 - 2 * rep
        self.offset = {(d, k): lax.rem(at[d] + sign * k + n, n) for d, n in SIZE.items() for k in range(-n // 2, n // 2) if k}

        def device(**moved):
            a = {**at, **moved}
            return (rep, (a["x"] * Y + a["y"]) * Z + a["z"])

        def ahead(d, k):
            return lax.rem(at[d] + SIZE[d] + k, SIZE[d])

        self.device = device
        self.beside = {(d, e): device(**{d: self.offset[d, e]}) for d in SIZE for e in (1, -1)}
        self.line = [ahead("z", k) for k in range(Z)]
        self.line_device = [device(z=to) for to in self.line]
        self.plane_device = [device(x=ahead("x", k // Y), y=ahead("y", k % Y)) for k in range(X * Y)]

    def off(self, dim, k):
        n = SIZE[dim]
        k = (k + n // 2) % n - n // 2
        return self.offset[dim, k] if k else self.at[dim]


def fence(p):
    peers = p.line_device[1:] + p.plane_device[1:]
    barrier = pltpu.get_barrier_semaphore()
    for peer in peers:
        pl.semaphore_signal(barrier, inc=1, device_id=peer, device_id_type=MESH)
    pl.semaphore_wait(barrier, len(peers))


class Loads:
    def __init__(self, p, terms, T, sem):
        self.p, self.terms, self.T, self.sem = p, terms, T, sem
        self.waited, self.left = set(), []
        for c, phase, _, d, k in REDUCE_ORDER:
            group = (c, d * k % lens(c)[0])
            if phase == 1 and group not in self.left:
                self.left.append(group)
        self.left += [(c, 0) for c in COLOURS]

    def start(self, count):
        p, (gate, up, down) = self.p, self.terms
        for c, k in self.left[:count]:
            j, T, s = p.off(DIMS[c][0], k), self.T[c], self.sem[c].at[k]
            if c == "A":
                for z in range(Z):
                    src = (gate, up)[z // X].at[z // 2 % 2, j, :, :, z % 2, pl.ds(0, LEFT)]
                    pltpu.make_async_copy(src, T.at[j, :, z], s).start()
            elif c == "B":
                for z in range(Z):
                    layer, q = down_place(z)
                    pltpu.make_async_copy(down.at[layer, :, j, q], T.at[j, z], s).start()
            else:
                layer, half = lax.rem(lax.div(j, 2), 2), lax.rem(j, 2)

                def load(ref):
                    pltpu.make_async_copy(ref.at[layer, :, :, :, half, pl.ds(LEFT, HALF - LEFT)], T.at[j], s).start()

                pl.when(j < X)(lambda: load(gate))
                pl.when(j >= X)(lambda: load(up))
        self.left = self.left[count:]

    def wait(self, c, k):
        k %= lens(c)[0]
        if (c, k) not in self.waited:
            self.waited.add((c, k))
            ref = self.T[c].at[self.p.off(DIMS[c][0], k)]
            pltpu.make_async_copy(ref, ref, self.sem[c].at[k]).wait()
            self.start(2)


class Reduce:
    def __init__(self, p, T, O, load, sent, arrived):
        self.p, self.T, self.O, self.load, self.sent, self.arrived = p, T, O, load, sent, arrived
        self.waited = set()


    def areas(self, t):
        c, phase, unit, d, k = t
        n1, n2, n3 = lens(c)
        d1, d2, d3 = DIMS[c]
        p = self.p
        slot = slots(SIZE[DIMS[c][phase - 1]], -ant_in(phase, unit))[d, k]
        if phase == 1:
            j2 = p.off(d2, unit[0])
            first, count = (0, n3) if unit[1] is None else (p.off(d3, unit[1]), 1)
            return (p.off(d1, d * k), j2), first, (slot, j2), first, count
        if phase == 2:
            j3 = p.off(d3, unit[0])
            return (p.at[d1], p.off(d2, d * k)), j3, (n1 - 1, slot), j3, 1
        return (p.at[d1], p.at[d2]), p.off(d3, d * k), (n1 - 1, n2 - 1), slot, 1

    def copy(self, t):
        c, phase, _, d, _ = t
        src, i, dst, j, n = self.areas(t)
        s = R_ID[t]
        return pltpu.make_async_remote_copy(
            src_ref=self.T[c].at[(*src, pl.ds(i, n))],
            dst_ref=self.O[c].at[(*dst, pl.ds(j, n))],
            send_sem=self.sent.at[S_ID[c, phase]],
            recv_sem=self.arrived.at[s],
            device_id=self.p.beside[DIMS[c][phase - 1], d],
            device_id_type=MESH,
        )

    def wait(self, t):
        if t not in self.waited:
            self.waited.add(t)
            self.copy(t).wait_recv()

    def ended(self, c, phase, j2, j3):
        last = lens(c)[0] - 1
        return [(0, j2, j3), (1, j2, j3), (last, 0, j3), (last, 1, j3)][: 2 * (phase - 1)]

    def send(self, t):
        c, phase, unit, d, k = t
        T, O = self.T[c], self.O[c]
        for w in REDUCE[t][2]:
            self.wait(w)
        self.load.wait(c, d * k if phase == 1 else 0)
        src, first, _, _, count = self.areas(t)
        before = (c, phase, unit, d, k + 1)
        chain = before in R_ID
        if phase > 1 or chain:
            _, _, there, start, _ = self.areas(before if chain else t)

            def one(i):
                parts = self.ended(c, phase, src[1], first + i)
                if chain:
                    parts.append((*there, start + i))
                total = T[(*src, first + i)].astype(F32)
                for part in parts:
                    total = total + O[part].astype(F32)
                T[(*src, first + i)] = total.astype(BF16)

            if count == 1:
                one(0)
            else:
                pl.loop(0, count)(one)
        self.copy(t).start()

    def own(self, c):
        n1, n2, _ = lens(c)
        for t in REDUCE:
            if t[0] == c and t[-1] == 1 and t[2] in ((), (0,), (0, 0)):
                self.wait(t)
        self.load.wait(c, 0)
        i, j, k = (self.p.at[d] for d in DIMS[c])
        total = self.T[c][i, j, k].astype(F32)
        for part in self.ended(c, 3, j, k) + [(n1 - 1, n2 - 1, e) for e in (0, 1)]:
            total = total + self.O[c][part].astype(F32)
        return total.astype(BF16).astype(F32)


class Gather:
    def __init__(self, p, O, sent, arrived):
        self.p, self.O, self.sent, self.arrived = p, O, sent, arrived
        self.waited = set()

    def copy(self, t, came=0):
        c, phase, unit, d, k = t
        d1, d2, d3 = DIMS[c]
        p, dim = self.p, DIMS[c][phase - 1]
        behind = p.off(dim, d * (1 - came - k))
        if phase == 1:
            at = (behind, p.off(d2, unit[0])) if unit[1] is None else (behind, p.off(d2, unit[0]), p.off(d3, unit[1]))
        else:
            at = (p.at[d1], behind, p.off(d3, unit[0])) if phase == 2 else (p.at[d1], p.at[d2], behind)
        ref, s = self.O[c].at[at], G_ID[t]
        return pltpu.make_async_remote_copy(
            src_ref=ref,
            dst_ref=ref,
            send_sem=self.sent.at[S_ID[c, phase]],
            recv_sem=self.arrived.at[s],
            device_id=p.beside[dim, d],
            device_id_type=MESH,
        )

    def wait(self, t):
        if t not in self.waited:
            self.waited.add(t)
            self.copy(t, 1).wait_recv()

    def send(self, t):
        for w in GATHER[t][2]:
            self.wait(w)
        self.copy(t).start()


def rows_of(a):
    return lax.broadcasted_iota(jnp.int32, a.shape, a.ndim - 2)


def joined(a, b, k):
    return pltpu.roll(jnp.where(rows_of(b) >= ROWS - k, a, b), k, b.ndim - 2)


def adamw(w, m, v, g):
    m = 0.9 * m + 0.1 * g
    v = 0.95 * v + 0.05 * g * g
    return w - 0.02 * (m * lax.rsqrt(v + 1e-8) + 0.1 * w), m, v


DOWN_ROWS = (ROWS, ROWS, ROWS // 2)
SCRATCH = {
    "raw": ((2, 2, HIGH, LAYERS, FF), F32),
    "raw_down": ((2, 20, LAYERS, D), F32),
    "own": ((HIGH, HALF, *TILE), F32),
    "own_low": ((PART, HIGH, *TILE), F32),
    "old": ((2, LAYERS, 2, 2, HALF, *TILE), BF16),
    "old_down": ((LAYERS, 3, HIGH, *TILE), BF16),
    "w": ((2, LAYERS, 2 * HALF, *TILE), F32),
    "w_low": ((LAYERS, 3, HIGH, *TILE), F32),
    "mv": ((2, 2, LAYERS, 2 * HALF, *TILE), F32),
    "mv_low": ((2, LAYERS, 3, HIGH, *TILE), F32),
    "out": ((Z, HALF, *TILE), BF16),
    "into": ((Z, HALF, *TILE), BF16),
    "out_low": ((2, 3, HIGH, *TILE), BF16),
    "into_low": ((LAYERS, 3, HIGH, *TILE), BF16),
    "new": ((Z, HALF, *TILE), BF16),
    "news": ((Z, HALF, *TILE), BF16),
    "new_low": ((LAYERS, 3, HIGH, *TILE), BF16),
    "news_low": ((2, 3, HIGH, *TILE), BF16),
    "z_sum": ((Z, *TILE), F32),
    "sum": ((X * Y, *TILE), F32),
}


class Few:
    def __init__(self, p, sent, arrived):
        self.p, self.sent, self.arrived, self.waits = p, sent, arrived, []

    def exchange(self, copies, get):
        i = len(self.waits)
        for src, dst, to in copies:
            one = pltpu.make_async_remote_copy(
                src_ref=src, dst_ref=dst, send_sem=self.sent.at[i], recv_sem=self.arrived.at[i], device_id=to, device_id_type=MESH
            )
            one.start()
        self.waits.append(pltpu.make_async_copy(get, get, self.sent.at[i]).wait)
        return pltpu.make_async_copy(get, get, self.arrived.at[i]).wait

    def line(self, out, into):
        p = self.p
        far = sorted(range(1, Z), key=lambda k: abs(k - X))
        return self.exchange([(out.at[p.line[k]], into.at[p.at["z"]], p.line_device[k]) for k in far], into.at[pl.ds(0, Z - 1)])

    def tell(self, ref, at, devices):
        return self.exchange([(ref.at[at], ref.at[at], to) for to in devices], ref.at[pl.ds(0, len(devices))])


def lanes(c):
    return pl.ds(pl.multiple_of(c * LANES, LANES), LANES)


def work(*refs):
    terms, weights, moments, refs = refs[:3], refs[3:6], refs[6:12], refs[12:]
    outs, made, refs = refs[:3], refs[3:9], refs[9:]
    O, T, refs = dict(zip(COLOURS, outs)), dict(zip(COLOURS, refs)), refs[3:]
    s = dict(zip(SCRATCH, refs))
    *load, small, sent, arrived, few_sent, few_arrived = refs[len(SCRATCH) :]
    p = Place()
    x, y, z = p.at.values()
    loads = Loads(p, terms, T, dict(zip(COLOURS, load)))
    loads.start(4)

    first = (X * Y * PART) * x + 20 * y + lax.div(PART * z, 2)
    for layer in range(LAYERS):
        for w in range(2):
            for i, row in enumerate((lax.max(z - 1, 0), lax.min(z, HIGH - 1))):
                pltpu.make_async_copy(weights[w].at[layer, x, y, row], s["old"].at[w, layer, i], small.at[0]).start()
        pltpu.make_async_copy(weights[2].at[layer, pl.ds(first, 3)], s["old_down"].at[layer], small.at[1]).start()
    for i in range(2):
        for w in range(2):
            pltpu.make_async_copy(moments[3 * i + w], s["raw"].at[i, w], small.at[2]).start()
        pltpu.make_async_copy(moments[3 * i + 2], s["raw_down"].at[i], small.at[3]).start()

    def rows_here():
        for i, name in enumerate(("old", "old_down", "raw", "raw_down")):
            pltpu.make_async_copy(s[name], s[name], small.at[i]).wait()

    chores, later = [rows_here], []

    def rows_in(w, layer):
        low, high = (s["old"][w, layer, i].reshape(2 * HALF, *TILE).astype(F32) for i in range(2))
        s["w"][w, layer] = joined(low, high, z)

    def rows_in_low(layer):
        part = [s["old_down"][layer, j].astype(F32) for j in range(3)]
        for j in range(3):
            s["w_low"][layer, j] = jnp.where(lax.rem(z, 2) == 1, joined(part[j], part[min(j + 1, 2)], ROWS // 2), part[j])

    def moments_in(i, w, layer):
        @pl.loop(0, 2 * HALF)
        def _(c):
            s["mv"][i, w, layer, c, pl.ds(0, HIGH)] = s["raw"][i, w, :, layer, lanes(c)]

    def moments_in_low(i, layer):
        @pl.loop(0, HIGH)
        def _(c):
            for j, n in enumerate(DOWN_ROWS):
                s["mv_low"][i, layer, j, c, pl.ds(0, n)] = s["raw_down"][i, pl.ds(ROWS * j, n), layer, lanes(c)]

    def moments_out(i, w, layer):
        @pl.loop(0, 2 * HALF)
        def _(c):
            rows = pl.ds(LAYERS * c + layer, HIGH, stride=LAYERS * 2 * HALF)
            made[3 * i + w][rows, :] = s["mv"][i, w, layer, c, pl.ds(0, HIGH)]

    def moments_out_low(i, layer):
        @pl.loop(0, HIGH)
        def _(c):
            for j, k in enumerate(DOWN_ROWS):
                rows = pl.ds(ROWS * j * LAYERS * HIGH + LAYERS * c + layer, k, stride=LAYERS * HIGH)
                made[3 * i + 2][rows, :] = s["mv_low"][i, layer, j, c, pl.ds(0, k)]

    for layer in range(LAYERS):
        for w in range(2):
            chores.append(functools.partial(rows_in, w, layer))
            for i in range(2):
                chores.append(functools.partial(moments_in, i, w, layer))
                later.append(functools.partial(moments_out, i, w, layer))
        chores.append(functools.partial(rows_in_low, layer))
        for i in range(2):
            chores.append(functools.partial(moments_in_low, i, layer))
            later.append(functools.partial(moments_out_low, i, layer))

    fence(p)
    reduce = Reduce(p, T, O, loads, sent, arrived)
    for n, t in enumerate(REDUCE_ORDER):
        reduce.send(t)
        if n > len(REDUCE_ORDER) // 4 and n % 4 == 0 and chores:
            chores.pop(0)()

    few = Few(p, few_sent, few_arrived)
    squares = jnp.zeros(TILE, F32)
    for c in COLOURS:
        g = reduce.own(c)
        if c == "B":
            s["own_low"][...] = g
        else:
            s["own"][:, pl.ds(*((0, LEFT) if c == "A" else (LEFT, HALF - LEFT)))] = g
        squares = squares + jnp.sum((g * g).reshape(tiles(c), *TILE), axis=0)
    s["z_sum"][z] = squares
    line_sums = few.tell(s["z_sum"], z, p.line_device[1:])

    for k in range(Z):
        at = s["own"][min(k, HIGH - 1)]
        s["out"][k] = (joined(s["own"][k - 1], at, k) if k else at).astype(BF16)
    pieces = few.line(s["out"], s["into"])
    s["into"][z] = s["out"][z]
    g = [s["own_low"][j] for j in range(PART)]
    for j in range(3):
        s["out_low"][0, j] = g[j].astype(BF16)
        s["out_low"][1, j] = joined(g[2 + j], g[min(3 + j, PART - 1)], ROWS // 2).astype(BF16)
    mine = lax.rem(z, 2)
    other, partner = 1 - mine, p.device(z=z + 1 - 2 * mine)
    pieces_low = few.exchange([(s["out_low"].at[other], s["into_low"].at[mine], partner)], s["into_low"].at[other])
    s["into_low"][mine] = s["out_low"][mine]

    line_sums()
    at = Y * x + y
    s["sum"][at] = jnp.sum(s["z_sum"][...], axis=0)
    sums = few.tell(s["sum"], at, p.plane_device[1:])
    pieces()
    pieces_low()
    sums()
    total = jnp.sum(s["sum"][...], axis=0)
    total = jnp.sum(jnp.sum(total, axis=1, keepdims=True), axis=0, keepdims=True)
    factor = jnp.minimum(1.0, 0.5 * lax.rsqrt(total / COUNT + 1e-30))

    for owner in range(Z):
        w, layer, part = owner // X, owner // 2 % 2, pl.ds(owner % 2 * HALF, HALF)
        g = s["into"][owner].astype(F32) * factor
        new, m, v = adamw(s["w"][w, layer, part], s["mv"][0, w, layer, part], s["mv"][1, w, layer, part], g)
        s["mv"][0, w, layer, part], s["mv"][1, w, layer, part] = m, v
        s["new"][owner] = new.astype(BF16)
    pieces = few.line(s["new"], s["news"])
    for layer in range(LAYERS):
        g = s["into_low"][layer].astype(F32) * factor
        new, m, v = adamw(s["w_low"][layer], s["mv_low"][0, layer], s["mv_low"][1, layer], g)
        s["mv_low"][0, layer], s["mv_low"][1, layer] = m, v
        s["new_low"][layer] = new.astype(BF16)
    pieces_low = few.exchange([(s["new_low"].at[other], s["news_low"].at[mine], partner)], s["news_low"].at[other])
    s["news_low"][mine] = s["new_low"][mine]
    s["news"][z] = s["new"][z]

    own = {c: tuple(p.at[d] for d in DIMS[c]) for c in COLOURS}

    def whole_low():
        pieces_low()
        a, b = ([s["news_low"][i, j].astype(F32) for j in range(3)] for i in range(2))
        seam = jnp.where(rows_of(b[0]) < ROWS // 2, a[2], pltpu.roll(b[0], ROWS // 2, 1))
        for i, tile in enumerate((a[0], a[1], seam, *(joined(b[j], b[j + 1], ROWS // 2) for j in range(2)))):
            O["B"][(*own["B"], i)] = tile.astype(BF16)

    def whole():
        pieces()
        t = [s["news"][k].astype(F32) for k in range(Z)]
        for i in range(HIGH):
            a = pltpu.roll(t[i], ROWS - i, 1) if i else t[i]
            tile = jnp.where(rows_of(a) < HIGH - i, a, pltpu.roll(t[i + 1], HIGH - i, 1)).astype(BF16)
            O["A"][(*own["A"], i)] = tile[:LEFT]
            O["C"][(*own["C"], i)] = tile[LEFT:]

    all_sent(T, sent)
    gather = Gather(p, O, sent, arrived)
    prepare = {"B": whole_low, "A": whole}
    for n, t in enumerate(GATHER_ORDER):
        needs = "B" if t[0] == "B" else "A"
        if needs in prepare:
            prepare.pop(needs)()
        gather.send(t)
        if n > len(GATHER_ORDER) // 4 and n % 4 == 0 and later:
            later.pop(0)()
    for t in ENDS:
        gather.wait(t)
    for wait in few.waits:
        wait()
    all_sent(T, sent)


def put(*refs):
    (a, b, c), moments, results, sem = refs[:3], refs[3:9], refs[9:18], refs[18]

    def copy(src, i, *at):
        pltpu.make_async_copy(src, results[i].at[at] if at else results[i], sem.at[i]).start()

    for z in range(Z):
        half, layer = z % 2, z // 2 % 2
        copy(a.at[:, :, z], z // X, layer, slice(None), slice(None), slice(None), half, pl.ds(0, LEFT))
        copy(c.at[z], z // X, layer, slice(None), slice(None), slice(None), half, pl.ds(LEFT, HALF - LEFT))
        layer, q = down_place(z)
        for y in range(Y):
            copy(b.at[y, z], 2, layer, slice(None), y, q)
    for i, moment in enumerate(moments):
        copy(moment, 3 + i)
    for i, ref in enumerate(results):
        pltpu.make_async_copy(ref, ref, sem.at[i]).wait()


def tiled(a, *cut):
    rows, columns = cut
    n = len(rows)
    a = a.reshape(LAYERS, *rows, ROWS, *columns, LANES)
    order = [*range(n + 1), *range(n + 2, n + 2 + len(columns)), n + 1, a.ndim - 1]
    return a.transpose(order)


def untiled(a, *cut):
    rows, columns = cut
    n = len(rows)
    order = [*range(n + 1), a.ndim - 2, *range(n + 1, a.ndim - 2), a.ndim - 1]
    a = a.transpose(order)
    return a.reshape(LAYERS, -1, a.shape[-1] * (HALF * 2 if len(columns) == 2 else HIGH))


WIDE, TALL = ((X, Y, HIGH), (2, HALF)), ((X, Y, X, PART), (HIGH,))


def unmoment(a, rows, columns):
    return a.reshape(rows, columns, LAYERS, LANES).transpose(0, 2, 1, 3).reshape(rows, LAYERS, columns * LANES).transpose(1, 0, 2)


def solution(mesh):
    shapes = [pltpu.VMEM((*lens(c), *BLOCK[c], *TILE), BF16) for c in COLOURS]
    hbm, vmem = pl.BlockSpec(memory_space=pltpu.HBM), pl.BlockSpec(memory_space=pltpu.VMEM)
    moment = (LAYERS * HIGH * HALF * 2, LANES)

    def semaphores(n):
        return pltpu.SemaphoreType.DMA((n,))

    def kernel(body, name, params, **more):
        return pl.pallas_call(body, name=name, compiler_params=pltpu.CompilerParams(**params), **more)

    def step(*arrays):
        terms, weights, moments = [t[0] for t in arrays[:3]], arrays[3:6], arrays[6:]
        wide = [tiled(a, *WIDE) for a in (*terms[:2], *weights[:2])]
        operands = [*wide[:2], tiled(terms[2], *TALL), *wide[2:], tiled(weights[2], (FF // ROWS,), (HIGH,))]
        operands += [a.transpose(1, 0, 2) for a in moments]
        made = kernel(
            work,
            "work",
            dict(collective_id=0, has_side_effects=True, vmem_limit_bytes=34 << 20),
            out_shape=(*shapes, *[pltpu.VMEM(moment, F32)] * 6),
            in_specs=[hbm] * 12,
            out_specs=[vmem] * 9,
            scratch_shapes=[
                *shapes,
                *(pltpu.VMEM(*a) for a in SCRATCH.values()),
                *(semaphores(lens(c)[0]) for c in COLOURS),
                semaphores(4),
                *(semaphores(n) for n in (len(S_ID), len(R_ID), 6, 6)),
            ],
        )(*(pltpu.with_memory_space_constraint(a, pltpu.HBM) for a in operands))
        out = kernel(
            put,
            "put",
            dict(vmem_limit_bytes=1 << 20),
            out_shape=[jax.ShapeDtypeStruct(a.shape, BF16) for a in operands[:3]] + [jax.ShapeDtypeStruct(moment, F32)] * 6,
            in_specs=[vmem] * 9,
            out_specs=[hbm] * 9,
            scratch_shapes=[semaphores(9)],
        )(*made)
        weights = [untiled(a, *cut) for a, cut in zip(out, (WIDE, WIDE, TALL))]
        return (*weights, *(unmoment(a, *m.shape[1:2], m.shape[2] // LANES) for a, m in zip(out[3:], moments)))

    all_of, cut = P(None, None, None), P(None, "dp", None)
    return jax.shard_map(
        step,
        mesh=mesh,
        in_specs=(P(("rep", "dp"), None, None, None),) * 3 + (all_of,) * 3 + (cut,) * 6,
        out_specs=(P("rep", None, None),) * 3 + (P("rep", "dp", None),) * 6,
        check_vma=False,
    )
```

```python
import functools

import jax
import jax.numpy as jnp
from jax import lax
from jax.experimental import pallas as pl
from jax.experimental.pallas import tpu as pltpu
from jax.sharding import PartitionSpec as P

MESH = pl.DeviceIdType.MESH
F32, BF16 = jnp.float32, jnp.bfloat16
X, Y, Z = 4, 4, 8
SIZE = {"x": X, "y": Y, "z": Z}
DIMS = {"A": ("x", "y", "z"), "B": ("y", "z", "x"), "C": ("z", "x", "y")}
COLOURS = tuple(DIMS)
LAYERS, ROWS, LANES = 2, 8, 128
TILE = (ROWS, LANES)
D, FF = 896, 2560
HIGH, HALF, LEFT, PART = 7, 10, 6, 5
BLOCK = {"A": (HIGH, LEFT), "B": (PART, HIGH), "C": (HIGH, HALF - LEFT)}
COUNT = 3 * LAYERS * D * FF


def lens(c):
    return tuple(SIZE[d] for d in DIMS[c])


def tiles(c):
    return BLOCK[c][0] * BLOCK[c][1]


def down_place(z):
    return z % 2, z // 2


def ring(n, ant):
    return [(ant, n // 2)] + [(d, k) for k in range(n // 2 - 1, 0, -1) for d in (1, -1)]


def slots(n, ant):
    return {m: i for i, m in enumerate(sorted(ring(n, ant), key=lambda m: (m[1], -m[0])))}


def far_first(n):
    return [n // 2] + [s * k for k in range(n // 2 - 1, 0, -1) for s in (1, -1)] + [0]


def ant_of(o):
    return -1 if o % 2 else 1


def ant_in(phase, unit):
    return (1, ant_of(sum(o for o in unit if o is not None)) if unit else 1)[phase < 3]


def came(c, phase, unit, n, o):
    far = n - o < n // 2 or (n == 2 * o and ant_in(phase, unit) == 1)
    return (c, phase, unit, 1, n - o) if far else (c, phase, unit, -1, o)


SECOND_BY_BLOCK, FIRST_BY_BLOCK = "AB", "A"


def gather_messages():
    out = {}
    for c in COLOURS:
        n1, n2, n3 = lens(c)

        def add(phase, unit, count, first):
            dim = DIMS[c][phase - 1]
            for d, k in ring(SIZE[dim], ant_in(phase, unit)):
                out[c, phase, unit, d, k] = ((dim, d), count * tiles(c), [(c, phase, unit, d, k - 1)] if k > 1 else first)

        blocks, whole = [(o,) for o in range(n3)], [(None,)]
        add(3, (), 1, [])
        line = [came(c, 3, (), n3, o) for o in range(1, n3)]
        second = blocks if c in SECOND_BY_BLOCK else whole
        for phase, head, chosen in ((2, (), second), (1, (0,), blocks if c in FIRST_BY_BLOCK else whole)):
            for unit in chosen:
                add(phase, head + unit, 1 if unit[0] is not None else n3, line[unit[0] - 1 : unit[0]] if unit[0] is not None else line)
        for o in range(1, n2):
            add(1, (o, None), n3, [came(c, 2, unit, n2, o) for unit in second])
    return out


def ordered(messages, slack, latency, rate):
    users, tail = {t: [] for t in messages}, {}
    for t, (_, _, waits) in messages.items():
        for w in waits:
            users[w].append(t)

    def way(t):
        if t not in tail:
            tail[t] = 2 * messages[t][1] / rate + latency + max((way(u) for u in users[t]), default=0)
        return tail[t]

    for t in messages:
        way(t)
    queues = {m[0]: [] for m in messages.values()}
    left, arrives, now, starts = list(messages), {}, 0.0, []
    while left or any(queues.values()):
        ready = [
            t
            for t in left
            if all(arrives.get(w, now + 1) <= now for w in messages[t][2])
            and 2 * sum(q[1] for q in queues[messages[t][0]]) <= slack
        ]
        if ready:
            t = max(ready, key=way)
            left.remove(t)
            starts.append(t)
            queues[messages[t][0]].append([t, messages[t][1] / rate])
            continue
        speed = {(m, d): 1 / 2 if queues[m, -d] else 1 for (m, d), q in queues.items() if q}
        full = {link: sum(q[1] for q in queues[link]) - slack / 2 for link in speed}
        events = [queues[link][0][1] / s for link, s in speed.items()] + [full[link] / s for link, s in speed.items() if full[link] > 0]
        pause = min(events + [a - now for a in arrives.values() if a > now]) + 1e-6
        now += pause
        for link, s in speed.items():
            queues[link][0][1] -= pause * s
            if queues[link][0][1] <= 0:
                arrives[queues[link].pop(0)[0]] = now + latency
    return starts, list(arrives)


GATHER = gather_messages()
GATHER_ORDER = ordered(GATHER, 1.0, 2.0, 60.0)[0]
ENDS = ordered(GATHER, 0.5, 3.0, 50.0)[1]
TURN = 67


def back(t):
    c, phase, unit, d, k = t
    return (c, phase, unit, -d, k)


REDUCE = {back(t): (link, n, []) for t, (link, n, _) in GATHER.items()}
for t, (_, _, waits) in GATHER.items():
    for w in waits:
        REDUCE[back(w)][2].append(back(t))
REDUCE_ORDER = [back(t) for t in reversed(ENDS)]
R_ID = {t: i for i, t in enumerate(REDUCE)}
G_ID = {t: R_ID[back(t)] for t in GATHER}
S_ID = {t: i for i, t in enumerate((c, phase) for c in COLOURS for phase in range(1, 4))}


def all_sent(T, sem):
    for (c, phase), i in S_ID.items():
        n = lens(c)[phase - 1] - 1
        ref = T[c].at[(*[0] * (phase - 1), pl.ds(0, n))]
        pltpu.make_async_copy(ref, ref, sem.at[i]).wait()


class Place:
    def __init__(self):
        dp = lax.axis_index("dp")
        rep = lax.axis_index("rep")
        self.at = at = {"x": lax.div(dp, Y * Z), "y": lax.rem(lax.div(dp, Z), Y), "z": lax.rem(dp, Z)}
        sign = 1 - 2 * rep
        self.offset = {(d, k): lax.rem(at[d] + sign * k + n, n) for d, n in SIZE.items() for k in range(-n // 2, n // 2) if k}

        def device(**moved):
            a = {**at, **moved}
            return (rep, (a["x"] * Y + a["y"]) * Z + a["z"])

        def ahead(d, k):
            return lax.rem(at[d] + SIZE[d] + k, SIZE[d])

        self.rep, self.device, self.twin = rep, device, (1 - rep, dp)
        self.beside = {(d, e): device(**{d: self.offset[d, e]}) for d in SIZE for e in (1, -1)}
        self.line = [ahead("z", k) for k in range(Z)]
        self.line_device = [device(z=to) for to in self.line]
        self.plane_device = [device(x=ahead("x", k // Y), y=ahead("y", k % Y)) for k in range(X * Y)]

    def off(self, dim, k):
        n = SIZE[dim]
        k = (k + n // 2) % n - n // 2
        return self.offset[dim, k] if k else self.at[dim]


def greet(p):
    peers = [*p.beside.values(), p.twin]
    barrier = pltpu.get_barrier_semaphore()
    for peer in peers:
        pl.semaphore_signal(barrier, inc=1, device_id=peer, device_id_type=MESH)
    return lambda: pl.semaphore_wait(barrier, len(peers))


class Loads:
    def __init__(self, p, terms, T, sem):
        self.p, self.terms, self.T, self.sem = p, terms, T, sem
        self.waited, self.left = set(), []
        for c, phase, _, d, k in REDUCE_ORDER:
            group = (c, d * k % lens(c)[0])
            if phase == 1 and group not in self.left:
                self.left.append(group)
        self.left += [(c, 0) for c in COLOURS]

    def start(self, count):
        p, (gate, up, down) = self.p, self.terms
        for c, k in self.left[:count]:
            j, T, s = p.off(DIMS[c][0], k), self.T[c], self.sem[c].at[k]
            if c == "A":
                for z in range(Z):
                    src = (gate, up)[z // X].at[z // 2 % 2, j, :, :, z % 2, pl.ds(0, LEFT)]
                    pltpu.make_async_copy(src, T.at[j, :, z], s).start()
            elif c == "B":
                for z in range(Z):
                    layer, q = down_place(z)
                    pltpu.make_async_copy(down.at[layer, :, j, q], T.at[j, z], s).start()
            else:
                layer, half = lax.rem(lax.div(j, 2), 2), lax.rem(j, 2)

                def load(ref):
                    pltpu.make_async_copy(ref.at[layer, :, :, :, half, pl.ds(LEFT, HALF - LEFT)], T.at[j], s).start()

                pl.when(j < X)(lambda: load(gate))
                pl.when(j >= X)(lambda: load(up))
        self.left = self.left[count:]

    def wait(self, c, k):
        k %= lens(c)[0]
        if (c, k) not in self.waited:
            self.waited.add((c, k))
            ref = self.T[c].at[self.p.off(DIMS[c][0], k)]
            pltpu.make_async_copy(ref, ref, self.sem[c].at[k]).wait()
            self.start(2)


class Reduce:
    def __init__(self, p, T, O, load, sent, arrived):
        self.p, self.T, self.O, self.load, self.sent, self.arrived = p, T, O, load, sent, arrived
        self.waited = set()


    def areas(self, t):
        c, phase, unit, d, k = t
        n1, n2, n3 = lens(c)
        d1, d2, d3 = DIMS[c]
        p = self.p
        slot = slots(SIZE[DIMS[c][phase - 1]], -ant_in(phase, unit))[d, k]
        if phase == 1:
            j2 = p.off(d2, unit[0])
            first, count = (0, n3) if unit[1] is None else (p.off(d3, unit[1]), 1)
            return (p.off(d1, d * k), j2), first, (slot, j2), first, count
        if phase == 2:
            first, count = (0, n3) if unit[0] is None else (p.off(d3, unit[0]), 1)
            return (p.at[d1], p.off(d2, d * k)), first, (n1 - 1, slot), first, count
        return (p.at[d1], p.at[d2]), p.off(d3, d * k), (n1 - 1, n2 - 1), slot, 1

    def copy(self, t):
        c, phase, _, d, _ = t
        src, i, dst, j, n = self.areas(t)
        s = R_ID[t]
        return pltpu.make_async_remote_copy(
            src_ref=self.T[c].at[(*src, pl.ds(i, n))],
            dst_ref=self.O[c].at[(*dst, pl.ds(j, n))],
            send_sem=self.sent.at[S_ID[c, phase]],
            recv_sem=self.arrived.at[s],
            device_id=self.p.beside[DIMS[c][phase - 1], d],
            device_id_type=MESH,
        )

    def wait(self, t):
        if t not in self.waited:
            self.waited.add(t)
            self.copy(t).wait_recv()

    def ended(self, c, phase, j2, j3):
        last = lens(c)[0] - 1
        return [(0, j2, j3), (1, j2, j3), (last, 0, j3), (last, 1, j3)][: 2 * (phase - 1)]

    def send(self, t):
        c, phase, unit, d, k = t
        T, O = self.T[c], self.O[c]
        for w in REDUCE[t][2]:
            self.wait(w)
        self.load.wait(c, d * k if phase == 1 else 0)
        src, first, _, _, count = self.areas(t)
        before = (c, phase, unit, d, k + 1)
        chain = before in R_ID
        if phase > 1 or chain:
            _, _, there, start, _ = self.areas(before if chain else t)

            def one(i):
                parts = self.ended(c, phase, src[1], first + i)
                if chain:
                    parts.append((*there, start + i))
                total = T[(*src, first + i)].astype(F32)
                for part in parts:
                    total = total + O[part].astype(F32)
                T[(*src, first + i)] = total.astype(BF16)

            if count == 1:
                one(0)
            else:
                pl.loop(0, count)(one)
        self.copy(t).start()

    def own(self, c):
        n1, n2, _ = lens(c)
        for t in REDUCE:
            if t[0] == c and t[-1] == 1 and not any(t[2]):
                self.wait(t)
        self.load.wait(c, 0)
        i, j, k = (self.p.at[d] for d in DIMS[c])
        total = self.T[c][i, j, k].astype(F32)
        for part in self.ended(c, 3, j, k) + [(n1 - 1, n2 - 1, e) for e in (0, 1)]:
            total = total + self.O[c][part].astype(F32)
        return total.astype(BF16).astype(F32)


class Gather:
    def __init__(self, p, O, sent, arrived):
        self.p, self.O, self.sent, self.arrived = p, O, sent, arrived
        self.waited = set()

    def copy(self, t, came=0):
        c, phase, unit, d, k = t
        d1, d2, d3 = DIMS[c]
        p, dim = self.p, DIMS[c][phase - 1]
        behind = p.off(dim, d * (1 - came - k))
        at = (behind, p.off(d2, unit[0])) if phase == 1 else (p.at[d1], behind) if phase == 2 else (p.at[d1], p.at[d2], behind)
        at += tuple(p.off(d3, o) for o in unit[-1:] if o is not None)
        ref, s = self.O[c].at[at], G_ID[t]
        return pltpu.make_async_remote_copy(
            src_ref=ref,
            dst_ref=ref,
            send_sem=self.sent.at[S_ID[c, phase]],
            recv_sem=self.arrived.at[s],
            device_id=p.beside[dim, d],
            device_id_type=MESH,
        )

    def wait(self, t):
        if t not in self.waited:
            self.waited.add(t)
            self.copy(t, 1).wait_recv()

    def send(self, t):
        for w in GATHER[t][2]:
            self.wait(w)
        self.copy(t).start()


def rows_of(a):
    return lax.broadcasted_iota(jnp.int32, a.shape, a.ndim - 2)


def joined(a, b, k):
    return pltpu.roll(jnp.where(rows_of(b) >= ROWS - k, a, b), k, b.ndim - 2)


def adamw(w, m, v, g):
    m = 0.9 * m + 0.1 * g
    v = 0.95 * v + 0.05 * g * g
    return w - 0.02 * (m * lax.rsqrt(v + 1e-8) + 0.1 * w), m, v


DOWN_ROWS = (ROWS, ROWS, ROWS // 2)
SCRATCH = {
    "raw": ((2, 2, HIGH, LAYERS, FF), F32),
    "raw_down": ((2, 20, LAYERS, D), F32),
    "own": ((HIGH, HALF, *TILE), F32),
    "own_low": ((PART, HIGH, *TILE), F32),
    "old": ((2, LAYERS, 2, 2, HALF, *TILE), BF16),
    "old_down": ((LAYERS, 3, HIGH, *TILE), BF16),
    "w": ((2, LAYERS, 2 * HALF, *TILE), F32),
    "w_low": ((LAYERS, 3, HIGH, *TILE), F32),
    "mv": ((2, 2, LAYERS, 2 * HALF, *TILE), F32),
    "mv_low": ((2, LAYERS, 3, HIGH, *TILE), F32),
    "out": ((Z, HALF, *TILE), BF16),
    "into": ((Z, HALF, *TILE), BF16),
    "out_low": ((2, 3, HIGH, *TILE), BF16),
    "into_low": ((LAYERS, 3, HIGH, *TILE), BF16),
    "new": ((Z, HALF, *TILE), BF16),
    "news": ((Z, HALF, *TILE), BF16),
    "new_low": ((LAYERS, 3, HIGH, *TILE), BF16),
    "news_low": ((2, 3, HIGH, *TILE), BF16),
    "z_sum": ((Z, *TILE), F32),
    "sum": ((X * Y, *TILE), F32),
}


class Few:
    def __init__(self, p, sent, arrived):
        self.p, self.sent, self.arrived, self.waits = p, sent, arrived, []

    def exchange(self, copies, get):
        i = len(self.waits)
        for src, dst, to in copies:
            one = pltpu.make_async_remote_copy(
                src_ref=src, dst_ref=dst, send_sem=self.sent.at[i], recv_sem=self.arrived.at[i], device_id=to, device_id_type=MESH
            )
            one.start()
        self.waits.append(pltpu.make_async_copy(get, get, self.sent.at[i]).wait)
        return pltpu.make_async_copy(get, get, self.arrived.at[i]).wait

    def line(self, out, into):
        p = self.p
        far = sorted(range(1, Z), key=lambda k: abs(k - X))
        return self.exchange([(out.at[p.line[k]], into.at[p.at["z"]], p.line_device[k]) for k in far], into.at[pl.ds(0, Z - 1)])

    def tell(self, ref, at, devices):
        return self.exchange([(ref.at[at], ref.at[at], to) for to in devices], ref.at[pl.ds(0, len(devices))])


def lanes(c):
    return pl.ds(pl.multiple_of(c * LANES, LANES), LANES)


def work(*refs):
    terms, weights, moments, refs = refs[:3], refs[3:6], refs[6:12], refs[12:]
    outs, made, refs = refs[:3], refs[3:9], refs[9:]
    O, T, refs = dict(zip(COLOURS, outs)), dict(zip(COLOURS, refs)), refs[3:]
    s = dict(zip(SCRATCH, refs))
    *load, small, turn, sent, arrived, few_sent, few_arrived = refs[len(SCRATCH) :]
    p = Place()
    x, y, z = p.at.values()
    all_here = greet(p)
    loads = Loads(p, terms, T, dict(zip(COLOURS, load)))
    loads.start(4)

    def rows_fetch():
        first = (X * Y * PART) * x + 20 * y + lax.div(PART * z, 2)
        for layer in range(LAYERS):
            for w in range(2):
                for i, row in enumerate((lax.max(z - 1, 0), lax.min(z, HIGH - 1))):
                    pltpu.make_async_copy(weights[w].at[layer, x, y, row], s["old"].at[w, layer, i], small.at[0]).start()
            pltpu.make_async_copy(weights[2].at[layer, pl.ds(first, 3)], s["old_down"].at[layer], small.at[1]).start()
        for i in range(2):
            for w in range(2):
                pltpu.make_async_copy(moments[3 * i + w], s["raw"].at[i, w], small.at[2]).start()
            pltpu.make_async_copy(moments[3 * i + 2], s["raw_down"].at[i], small.at[3]).start()

    def rows_here():
        for i, name in enumerate(("old", "old_down", "raw", "raw_down")):
            pltpu.make_async_copy(s[name], s[name], small.at[i]).wait()

    chores, later = [rows_fetch, rows_here], []

    def rows_in(w, layer):
        low, high = (s["old"][w, layer, i].reshape(2 * HALF, *TILE).astype(F32) for i in range(2))
        s["w"][w, layer] = joined(low, high, z)

    def rows_in_low(layer):
        part = [s["old_down"][layer, j].astype(F32) for j in range(3)]
        for j in range(3):
            s["w_low"][layer, j] = jnp.where(lax.rem(z, 2) == 1, joined(part[j], part[min(j + 1, 2)], ROWS // 2), part[j])

    def moments_in(i, w, layer):
        @pl.loop(0, 2 * HALF)
        def _(c):
            s["mv"][i, w, layer, c, pl.ds(0, HIGH)] = s["raw"][i, w, :, layer, lanes(c)]

    def moments_in_low(i, layer):
        @pl.loop(0, HIGH)
        def _(c):
            for j, n in enumerate(DOWN_ROWS):
                s["mv_low"][i, layer, j, c, pl.ds(0, n)] = s["raw_down"][i, pl.ds(ROWS * j, n), layer, lanes(c)]

    def moments_out(i, w, layer):
        @pl.loop(0, 2 * HALF)
        def _(c):
            rows = pl.ds(LAYERS * c + layer, HIGH, stride=LAYERS * 2 * HALF)
            made[3 * i + w][rows, :] = s["mv"][i, w, layer, c, pl.ds(0, HIGH)]

    def moments_out_low(i, layer):
        @pl.loop(0, HIGH)
        def _(c):
            for j, k in enumerate(DOWN_ROWS):
                rows = pl.ds(ROWS * j * LAYERS * HIGH + LAYERS * c + layer, k, stride=LAYERS * HIGH)
                made[3 * i + 2][rows, :] = s["mv_low"][i, layer, j, c, pl.ds(0, k)]

    for layer in range(LAYERS):
        for w in range(2):
            chores.append(functools.partial(rows_in, w, layer))
            for i in range(2):
                chores.append(functools.partial(moments_in, i, w, layer))
                later.append(functools.partial(moments_out, i, w, layer))
        chores.append(functools.partial(rows_in_low, layer))
        for i in range(2):
            chores.append(functools.partial(moments_in_low, i, layer))
            later.append(functools.partial(moments_out_low, i, layer))

    all_here()
    reduce = Reduce(p, T, O, loads, sent, arrived)
    pl.when(p.rep == 0)(lambda: pl.semaphore_wait(turn, 1))
    for n, t in enumerate(REDUCE_ORDER):
        reduce.send(t)
        if n == TURN:
            pl.when(p.rep == 1)(lambda: pl.semaphore_signal(turn, inc=1, device_id=p.twin, device_id_type=MESH))
        if n > len(REDUCE_ORDER) // 4 and n % 4 == 0 and chores:
            chores.pop(0)()

    few = Few(p, few_sent, few_arrived)
    squares = jnp.zeros(TILE, F32)
    for c in COLOURS:
        g = reduce.own(c)
        if c == "B":
            s["own_low"][...] = g
        else:
            s["own"][:, pl.ds(*((0, LEFT) if c == "A" else (LEFT, HALF - LEFT)))] = g
        squares = squares + jnp.sum((g * g).reshape(tiles(c), *TILE), axis=0)
    s["z_sum"][z] = squares
    line_sums = few.tell(s["z_sum"], z, p.line_device[1:])

    for k in range(Z):
        at = s["own"][min(k, HIGH - 1)]
        s["out"][k] = (joined(s["own"][k - 1], at, k) if k else at).astype(BF16)
    pieces = few.line(s["out"], s["into"])
    s["into"][z] = s["out"][z]
    g = [s["own_low"][j] for j in range(PART)]
    for j in range(3):
        s["out_low"][0, j] = g[j].astype(BF16)
        s["out_low"][1, j] = joined(g[2 + j], g[min(3 + j, PART - 1)], ROWS // 2).astype(BF16)
    mine = lax.rem(z, 2)
    other, partner = 1 - mine, p.device(z=z + 1 - 2 * mine)
    pieces_low = few.exchange([(s["out_low"].at[other], s["into_low"].at[mine], partner)], s["into_low"].at[other])
    s["into_low"][mine] = s["out_low"][mine]

    line_sums()
    at = Y * x + y
    s["sum"][at] = jnp.sum(s["z_sum"][...], axis=0)
    sums = few.tell(s["sum"], at, p.plane_device[1:])
    pieces()
    pieces_low()
    sums()
    total = jnp.sum(s["sum"][...], axis=0)
    total = jnp.sum(jnp.sum(total, axis=1, keepdims=True), axis=0, keepdims=True)
    factor = jnp.minimum(1.0, 0.5 * lax.rsqrt(total / COUNT + 1e-30))

    for owner in range(Z):
        w, layer, part = owner // X, owner // 2 % 2, pl.ds(owner % 2 * HALF, HALF)
        g = s["into"][owner].astype(F32) * factor
        new, m, v = adamw(s["w"][w, layer, part], s["mv"][0, w, layer, part], s["mv"][1, w, layer, part], g)
        s["mv"][0, w, layer, part], s["mv"][1, w, layer, part] = m, v
        s["new"][owner] = new.astype(BF16)
    pieces = few.line(s["new"], s["news"])
    for layer in range(LAYERS):
        g = s["into_low"][layer].astype(F32) * factor
        new, m, v = adamw(s["w_low"][layer], s["mv_low"][0, layer], s["mv_low"][1, layer], g)
        s["mv_low"][0, layer], s["mv_low"][1, layer] = m, v
        s["new_low"][layer] = new.astype(BF16)
    pieces_low = few.exchange([(s["new_low"].at[other], s["news_low"].at[mine], partner)], s["news_low"].at[other])
    s["news_low"][mine] = s["new_low"][mine]
    s["news"][z] = s["new"][z]

    own = {c: tuple(p.at[d] for d in DIMS[c]) for c in COLOURS}

    def whole_low():
        pieces_low()
        a, b = ([s["news_low"][i, j].astype(F32) for j in range(3)] for i in range(2))
        seam = jnp.where(rows_of(b[0]) < ROWS // 2, a[2], pltpu.roll(b[0], ROWS // 2, 1))
        for i, tile in enumerate((a[0], a[1], seam, *(joined(b[j], b[j + 1], ROWS // 2) for j in range(2)))):
            O["B"][(*own["B"], i)] = tile.astype(BF16)

    def whole():
        pieces()
        t = [s["news"][k].astype(F32) for k in range(Z)]
        for i in range(HIGH):
            a = pltpu.roll(t[i], ROWS - i, 1) if i else t[i]
            tile = jnp.where(rows_of(a) < HIGH - i, a, pltpu.roll(t[i + 1], HIGH - i, 1)).astype(BF16)
            O["A"][(*own["A"], i)] = tile[:LEFT]
            O["C"][(*own["C"], i)] = tile[LEFT:]

    all_sent(T, sent)
    gather = Gather(p, O, sent, arrived)
    prepare = {"B": whole_low, "A": whole}
    for n, t in enumerate(GATHER_ORDER):
        needs = "B" if t[0] == "B" else "A"
        if needs in prepare:
            prepare.pop(needs)()
        gather.send(t)
        if n > len(GATHER_ORDER) // 4 and n % 4 == 0 and later:
            later.pop(0)()
    for t in ENDS:
        gather.wait(t)
    for wait in few.waits:
        wait()
    all_sent(T, sent)


def put(*refs):
    (a, b, c), moments, results, sem = refs[:3], refs[3:9], refs[9:18], refs[18]

    def copy(src, i, *at):
        pltpu.make_async_copy(src, results[i].at[at] if at else results[i], sem.at[i]).start()

    for z in range(Z):
        half, layer = z % 2, z // 2 % 2
        copy(a.at[:, :, z], z // X, layer, slice(None), slice(None), slice(None), half, pl.ds(0, LEFT))
        copy(c.at[z], z // X, layer, slice(None), slice(None), slice(None), half, pl.ds(LEFT, HALF - LEFT))
        layer, q = down_place(z)
        for y in range(Y):
            copy(b.at[y, z], 2, layer, slice(None), y, q)
    for i, moment in enumerate(moments):
        copy(moment, 3 + i)
    for i, ref in enumerate(results):
        pltpu.make_async_copy(ref, ref, sem.at[i]).wait()


def tiled(a, *cut):
    rows, columns = cut
    n = len(rows)
    a = a.reshape(LAYERS, *rows, ROWS, *columns, LANES)
    order = [*range(n + 1), *range(n + 2, n + 2 + len(columns)), n + 1, a.ndim - 1]
    return a.transpose(order)


def untiled(a, *cut):
    rows, columns = cut
    n = len(rows)
    order = [*range(n + 1), a.ndim - 2, *range(n + 1, a.ndim - 2), a.ndim - 1]
    a = a.transpose(order)
    return a.reshape(LAYERS, -1, a.shape[-1] * (HALF * 2 if len(columns) == 2 else HIGH))


WIDE, TALL = ((X, Y, HIGH), (2, HALF)), ((X, Y, X, PART), (HIGH,))


def unmoment(a, rows, columns):
    return a.reshape(rows, columns, LAYERS, LANES).transpose(0, 2, 1, 3).reshape(rows, LAYERS, columns * LANES).transpose(1, 0, 2)


def solution(mesh):
    shapes = [pltpu.VMEM((*lens(c), *BLOCK[c], *TILE), BF16) for c in COLOURS]
    hbm, vmem = pl.BlockSpec(memory_space=pltpu.HBM), pl.BlockSpec(memory_space=pltpu.VMEM)
    moment = (LAYERS * HIGH * HALF * 2, LANES)

    def semaphores(n):
        return pltpu.SemaphoreType.DMA((n,))

    def kernel(body, name, params, **more):
        return pl.pallas_call(body, name=name, compiler_params=pltpu.CompilerParams(**params), **more)

    def step(*arrays):
        terms, weights, moments = [t[0] for t in arrays[:3]], arrays[3:6], arrays[6:]
        wide = [tiled(a, *WIDE) for a in (*terms[:2], *weights[:2])]
        operands = [*wide[:2], tiled(terms[2], *TALL), *wide[2:], tiled(weights[2], (FF // ROWS,), (HIGH,))]
        operands += [a.transpose(1, 0, 2) for a in moments]
        made = kernel(
            work,
            "work",
            dict(collective_id=0, has_side_effects=True, vmem_limit_bytes=34 << 20),
            out_shape=(*shapes, *[pltpu.VMEM(moment, F32)] * 6),
            in_specs=[hbm] * 12,
            out_specs=[vmem] * 9,
            scratch_shapes=[
                *shapes,
                *(pltpu.VMEM(*a) for a in SCRATCH.values()),
                *(semaphores(lens(c)[0]) for c in COLOURS),
                semaphores(4),
                pltpu.SemaphoreType.REGULAR,
                *(semaphores(n) for n in (len(S_ID), len(R_ID), 6, 6)),
            ],
        )(*(pltpu.with_memory_space_constraint(a, pltpu.HBM) for a in operands))
        out = kernel(
            put,
            "put",
            dict(vmem_limit_bytes=1 << 20),
            out_shape=[jax.ShapeDtypeStruct(a.shape, BF16) for a in operands[:3]] + [jax.ShapeDtypeStruct(moment, F32)] * 6,
            in_specs=[vmem] * 9,
            out_specs=[hbm] * 9,
            scratch_shapes=[semaphores(9)],
        )(*made)
        weights = [untiled(a, *cut) for a, cut in zip(out, (WIDE, WIDE, TALL))]
        return (*weights, *(unmoment(a, *m.shape[1:2], m.shape[2] // LANES) for a, m in zip(out[3:], moments)))

    all_of, cut = P(None, None, None), P(None, "dp", None)
    return jax.shard_map(
        step,
        mesh=mesh,
        in_specs=(P(("rep", "dp"), None, None, None),) * 3 + (all_of,) * 3 + (cut,) * 6,
        out_specs=(P("rep", None, None),) * 3 + (P("rep", "dp", None),) * 6,
        check_vma=False,
    )
```

```python
import functools

import jax
import jax.numpy as jnp
from jax import lax
from jax.experimental import pallas as pl
from jax.experimental.pallas import tpu as pltpu
from jax.sharding import PartitionSpec as P

MESH = pl.DeviceIdType.MESH
F32, BF16 = jnp.float32, jnp.bfloat16
X, Y, Z = 4, 4, 8
SIZE = {"x": X, "y": Y, "z": Z}
DIMS = {"A": ("x", "y", "z"), "B": ("y", "z", "x"), "C": ("z", "x", "y")}
COLOURS = tuple(DIMS)
LAYERS, ROWS, LANES = 2, 8, 128
TILE = (ROWS, LANES)
D, FF = 896, 2560
HIGH, HALF, LEFT, PART = 7, 10, 6, 5
BLOCK = {"A": (HIGH, LEFT), "B": (PART, HIGH), "C": (HIGH, HALF - LEFT)}
COUNT = 3 * LAYERS * D * FF


def lens(c):
    return tuple(SIZE[d] for d in DIMS[c])


def tiles(c):
    return BLOCK[c][0] * BLOCK[c][1]


def down_place(z):
    return z % 2, z // 2


def ring(n, ant):
    return [(ant, n // 2)] + [(d, k) for k in range(n // 2 - 1, 0, -1) for d in (1, -1)]


def slots(n, ant):
    return {m: i for i, m in enumerate(sorted(ring(n, ant), key=lambda m: (m[1], -m[0])))}


def far_first(n):
    return [n // 2] + [s * k for k in range(n // 2 - 1, 0, -1) for s in (1, -1)] + [0]


def ant_of(o):
    return -1 if o % 2 else 1


def ant_in(phase, unit):
    return (1, ant_of(sum(o for o in unit if o is not None)) if unit else 1)[phase < 3]


def came(c, phase, unit, n, o):
    far = n - o < n // 2 or (n == 2 * o and ant_in(phase, unit) == 1)
    return (c, phase, unit, 1, n - o) if far else (c, phase, unit, -1, o)


SECOND_BY_BLOCK, FIRST_BY_BLOCK = "AB", "A"


def gather_messages():
    out = {}
    for c in COLOURS:
        n1, n2, n3 = lens(c)

        def add(phase, unit, count, first):
            dim = DIMS[c][phase - 1]
            for d, k in ring(SIZE[dim], ant_in(phase, unit)):
                out[c, phase, unit, d, k] = ((dim, d), count * tiles(c), [(c, phase, unit, d, k - 1)] if k > 1 else first)

        blocks, whole = [(o,) for o in range(n3)], [(None,)]
        add(3, (), 1, [])
        line = [came(c, 3, (), n3, o) for o in range(1, n3)]
        second = blocks if c in SECOND_BY_BLOCK else whole
        for phase, head, chosen in ((2, (), second), (1, (0,), blocks if c in FIRST_BY_BLOCK else whole)):
            for unit in chosen:
                add(phase, head + unit, 1 if unit[0] is not None else n3, line[unit[0] - 1 : unit[0]] if unit[0] is not None else line)
        for o in range(1, n2):
            add(1, (o, None), n3, [came(c, 2, unit, n2, o) for unit in second])
    return out


def ordered(messages, slack, latency, rate):
    users, tail = {t: [] for t in messages}, {}
    for t, (_, _, waits) in messages.items():
        for w in waits:
            users[w].append(t)

    def way(t):
        if t not in tail:
            tail[t] = 2 * messages[t][1] / rate + latency + max((way(u) for u in users[t]), default=0)
        return tail[t]

    for t in messages:
        way(t)
    queues = {m[0]: [] for m in messages.values()}
    left, arrives, now, starts = list(messages), {}, 0.0, []
    while left or any(queues.values()):
        ready = [
            t
            for t in left
            if all(arrives.get(w, now + 1) <= now for w in messages[t][2])
            and 2 * sum(q[1] for q in queues[messages[t][0]]) <= slack
        ]
        if ready:
            t = max(ready, key=way)
            left.remove(t)
            starts.append(t)
            queues[messages[t][0]].append([t, messages[t][1] / rate])
            continue
        speed = {(m, d): 1 / 2 if queues[m, -d] else 1 for (m, d), q in queues.items() if q}
        full = {link: sum(q[1] for q in queues[link]) - slack / 2 for link in speed}
        events = [queues[link][0][1] / s for link, s in speed.items()] + [full[link] / s for link, s in speed.items() if full[link] > 0]
        pause = min(events + [a - now for a in arrives.values() if a > now]) + 1e-6
        now += pause
        for link, s in speed.items():
            queues[link][0][1] -= pause * s
            if queues[link][0][1] <= 0:
                arrives[queues[link].pop(0)[0]] = now + latency
    return starts, list(arrives)


GATHER = gather_messages()
GATHER_ORDER, GATHER_ENDS = ordered(GATHER, 1.0, 2.0, 60.0)
ENDS = ordered(GATHER, 0.5, 3.0, 50.0)[1]
TURN = 67
AHEAD = 12


def back(t):
    c, phase, unit, d, k = t
    return (c, phase, unit, -d, k)


REDUCE = {back(t): (link, n, []) for t, (link, n, _) in GATHER.items()}
for t, (_, _, waits) in GATHER.items():
    for w in waits:
        REDUCE[back(w)][2].append(back(t))
REDUCE_ORDER = [back(t) for t in reversed(ENDS)]
R_ID = {t: i for i, t in enumerate(REDUCE)}
G_ID = {t: R_ID[back(t)] for t in GATHER}
S_ID = {t: i for i, t in enumerate((c, phase) for c in COLOURS for phase in range(1, 4))}


def all_sent(T, sem):
    for (c, phase), i in S_ID.items():
        n = lens(c)[phase - 1] - 1
        ref = T[c].at[(*[0] * (phase - 1), pl.ds(0, n))]
        pltpu.make_async_copy(ref, ref, sem.at[i]).wait()


class Place:
    def __init__(self):
        dp = lax.axis_index("dp")
        rep = lax.axis_index("rep")
        self.at = at = {"x": lax.div(dp, Y * Z), "y": lax.rem(lax.div(dp, Z), Y), "z": lax.rem(dp, Z)}
        sign = 1 - 2 * rep
        self.offset = {(d, k): lax.rem(at[d] + sign * k + n, n) for d, n in SIZE.items() for k in range(-n // 2, n // 2) if k}

        def device(**moved):
            a = {**at, **moved}
            return (rep, (a["x"] * Y + a["y"]) * Z + a["z"])

        def ahead(d, k):
            return lax.rem(at[d] + SIZE[d] + k, SIZE[d])

        self.rep, self.device, self.twin = rep, device, (1 - rep, dp)
        self.beside = {(d, e): device(**{d: self.offset[d, e]}) for d in SIZE for e in (1, -1)}
        self.line = [ahead("z", k) for k in range(Z)]
        self.line_device = [device(z=to) for to in self.line]
        self.plane_device = [device(x=ahead("x", k // Y), y=ahead("y", k % Y)) for k in range(X * Y)]

    def off(self, dim, k):
        n = SIZE[dim]
        k = (k + n // 2) % n - n // 2
        return self.offset[dim, k] if k else self.at[dim]


def greet(p):
    peers = [*p.beside.values(), p.twin]
    barrier = pltpu.get_barrier_semaphore()
    for peer in peers:
        pl.semaphore_signal(barrier, inc=1, device_id=peer, device_id_type=MESH)
    return lambda: pl.semaphore_wait(barrier, len(peers))


def block_of(t):
    c, phase, unit, d, k = t
    n1, n2, _ = lens(c)
    return (c, d * k % n1, unit[0] % n2) if phase == 1 else (c, 0, d * k % n2 if phase == 2 else 0)


class Loads:
    def __init__(self, p, terms, T, sem):
        self.p, self.terms, self.T, self.sem = p, terms, T, sem
        self.left = list(dict.fromkeys([block_of(t) for t in REDUCE_ORDER] + [(c, 0, 0) for c in COLOURS]))
        self.place = {part: i % AHEAD for i, part in enumerate(self.left)}

    def at(self, part):
        c, k, o = part
        return self.p.off(DIMS[c][0], k), self.p.off(DIMS[c][1], o)

    def start(self, count):
        gate, up, down = self.terms
        for part in self.left[:count]:
            c, (i, j), s = part[0], self.at(part), self.sem.at[self.place[part]]
            T = self.T[c].at[i, j]
            if c == "A":
                for z in range(Z):
                    src = (gate, up)[z // X].at[z // 2 % 2, i, j, :, z % 2, pl.ds(0, LEFT)]
                    pltpu.make_async_copy(src, T.at[z], s).start()
            elif c == "B":
                pltpu.make_async_copy(down.at[lax.rem(j, 2), :, i, lax.div(j, 2)], T, s).start()
            else:
                layer, half = lax.rem(lax.div(i, 2), 2), lax.rem(i, 2)

                def load(ref):
                    pltpu.make_async_copy(ref.at[layer, j, :, :, half, pl.ds(LEFT, HALF - LEFT)], T, s).start()

                pl.when(i < X)(lambda: load(gate))
                pl.when(i >= X)(lambda: load(up))
        self.left = self.left[count:]

    def wait(self, part):
        if part in self.place:
            ref = self.T[part[0]].at[self.at(part)]
            pltpu.make_async_copy(ref, ref, self.sem.at[self.place.pop(part)]).wait()
            self.start(1)


class Reduce:
    def __init__(self, p, T, O, load, sent, arrived):
        self.p, self.T, self.O, self.load, self.sent, self.arrived = p, T, O, load, sent, arrived
        self.waited = set()


    def areas(self, t):
        c, phase, unit, d, k = t
        n1, n2, n3 = lens(c)
        d1, d2, d3 = DIMS[c]
        p = self.p
        slot = slots(SIZE[DIMS[c][phase - 1]], -ant_in(phase, unit))[d, k]
        if phase == 1:
            j2 = p.off(d2, unit[0])
            first, count = (0, n3) if unit[1] is None else (p.off(d3, unit[1]), 1)
            return (p.off(d1, d * k), j2), first, (slot, j2), first, count
        if phase == 2:
            first, count = (0, n3) if unit[0] is None else (p.off(d3, unit[0]), 1)
            return (p.at[d1], p.off(d2, d * k)), first, (n1 - 1, slot), first, count
        return (p.at[d1], p.at[d2]), p.off(d3, d * k), (n1 - 1, n2 - 1), slot, 1

    def copy(self, t):
        c, phase, _, d, _ = t
        src, i, dst, j, n = self.areas(t)
        s = R_ID[t]
        return pltpu.make_async_remote_copy(
            src_ref=self.T[c].at[(*src, pl.ds(i, n))],
            dst_ref=self.O[c].at[(*dst, pl.ds(j, n))],
            send_sem=self.sent.at[S_ID[c, phase]],
            recv_sem=self.arrived.at[s],
            device_id=self.p.beside[DIMS[c][phase - 1], d],
            device_id_type=MESH,
        )

    def wait(self, t):
        if t not in self.waited:
            self.waited.add(t)
            self.copy(t).wait_recv()

    def ended(self, c, phase, j2, j3):
        last = lens(c)[0] - 1
        return [(0, j2, j3), (1, j2, j3), (last, 0, j3), (last, 1, j3)][: 2 * (phase - 1)]

    def send(self, t):
        c, phase, unit, d, k = t
        T, O = self.T[c], self.O[c]
        for w in REDUCE[t][2]:
            self.wait(w)
        self.load.wait(block_of(t))
        src, first, _, _, count = self.areas(t)
        before = (c, phase, unit, d, k + 1)
        chain = before in R_ID
        if phase > 1 or chain:
            _, _, there, start, _ = self.areas(before if chain else t)

            def one(i):
                parts = self.ended(c, phase, src[1], first + i)
                if chain:
                    parts.append((*there, start + i))
                total = T[(*src, first + i)].astype(F32)
                for part in parts:
                    total = total + O[part].astype(F32)
                T[(*src, first + i)] = total.astype(BF16)

            if count == 1:
                one(0)
            else:
                pl.loop(0, count)(one)
        self.copy(t).start()

    def own(self, c):
        n1, n2, _ = lens(c)
        for t in REDUCE:
            if t[0] == c and t[-1] == 1 and not any(t[2]):
                self.wait(t)
        self.load.wait((c, 0, 0))
        i, j, k = (self.p.at[d] for d in DIMS[c])
        total = self.T[c][i, j, k].astype(F32)
        for part in self.ended(c, 3, j, k) + [(n1 - 1, n2 - 1, e) for e in (0, 1)]:
            total = total + self.O[c][part].astype(F32)
        return total.astype(BF16).astype(F32)


class Gather:
    def __init__(self, p, O, sent, arrived):
        self.p, self.O, self.sent, self.arrived = p, O, sent, arrived
        self.waited = set()

    def copy(self, t, came=0):
        c, phase, unit, d, k = t
        d1, d2, d3 = DIMS[c]
        p, dim = self.p, DIMS[c][phase - 1]
        behind = p.off(dim, d * (1 - came - k))
        at = (behind, p.off(d2, unit[0])) if phase == 1 else (p.at[d1], behind) if phase == 2 else (p.at[d1], p.at[d2], behind)
        at += tuple(p.off(d3, o) for o in unit[-1:] if o is not None)
        ref, s = self.O[c].at[at], G_ID[t]
        return pltpu.make_async_remote_copy(
            src_ref=ref,
            dst_ref=ref,
            send_sem=self.sent.at[S_ID[c, phase]],
            recv_sem=self.arrived.at[s],
            device_id=p.beside[dim, d],
            device_id_type=MESH,
        )

    def wait(self, t):
        if t not in self.waited:
            self.waited.add(t)
            self.copy(t, 1).wait_recv()

    def send(self, t):
        for w in GATHER[t][2]:
            self.wait(w)
        self.copy(t).start()


def rows_of(a):
    return lax.broadcasted_iota(jnp.int32, a.shape, a.ndim - 2)


def joined(a, b, k):
    return pltpu.roll(jnp.where(rows_of(b) >= ROWS - k, a, b), k, b.ndim - 2)


def adamw(w, m, v, g):
    m = 0.9 * m + 0.1 * g
    v = 0.95 * v + 0.05 * g * g
    return w - 0.02 * (m * lax.rsqrt(v + 1e-8) + 0.1 * w), m, v


DOWN_ROWS = (ROWS, ROWS, ROWS // 2)
SCRATCH = {
    "raw": ((2, 2, HIGH, LAYERS, FF), F32),
    "raw_down": ((2, 20, LAYERS, D), F32),
    "own": ((HIGH, HALF, *TILE), F32),
    "own_low": ((PART, HIGH, *TILE), F32),
    "old": ((2, LAYERS, 2, 2, HALF, *TILE), BF16),
    "old_down": ((LAYERS, 3, HIGH, *TILE), BF16),
    "w": ((2, LAYERS, 2 * HALF, *TILE), F32),
    "w_low": ((LAYERS, 3, HIGH, *TILE), F32),
    "mv": ((2, 2, LAYERS, 2 * HALF, *TILE), F32),
    "mv_low": ((2, LAYERS, 3, HIGH, *TILE), F32),
    "out": ((Z, HALF, *TILE), BF16),
    "into": ((Z, HALF, *TILE), BF16),
    "out_low": ((2, 3, HIGH, *TILE), BF16),
    "into_low": ((LAYERS, 3, HIGH, *TILE), BF16),
    "new": ((Z, HALF, *TILE), BF16),
    "news": ((Z, HALF, *TILE), BF16),
    "new_low": ((LAYERS, 3, HIGH, *TILE), BF16),
    "news_low": ((2, 3, HIGH, *TILE), BF16),
    "z_sum": ((Z, *TILE), F32),
    "sum": ((X * Y, *TILE), F32),
}


class Few:
    def __init__(self, p, sent, arrived):
        self.p, self.sent, self.arrived, self.waits = p, sent, arrived, []

    def exchange(self, copies, get):
        i = len(self.waits)
        for src, dst, to in copies:
            one = pltpu.make_async_remote_copy(
                src_ref=src, dst_ref=dst, send_sem=self.sent.at[i], recv_sem=self.arrived.at[i], device_id=to, device_id_type=MESH
            )
            one.start()
        self.waits.append(pltpu.make_async_copy(get, get, self.sent.at[i]).wait)
        return pltpu.make_async_copy(get, get, self.arrived.at[i]).wait

    def line(self, out, into):
        p = self.p
        far = sorted(range(1, Z), key=lambda k: abs(k - X))
        return self.exchange([(out.at[p.line[k]], into.at[p.at["z"]], p.line_device[k]) for k in far], into.at[pl.ds(0, Z - 1)])

    def tell(self, ref, at, devices):
        return self.exchange([(ref.at[at], ref.at[at], to) for to in devices], ref.at[pl.ds(0, len(devices))])


def lanes(c):
    return pl.ds(pl.multiple_of(c * LANES, LANES), LANES)


def work(*refs):
    terms, weights, moments, refs = refs[:3], refs[3:6], refs[6:12], refs[12:]
    outs, made, refs = refs[:3], refs[3:9], refs[9:]
    O, T, refs = dict(zip(COLOURS, outs)), dict(zip(COLOURS, refs)), refs[3:]
    s = dict(zip(SCRATCH, refs))
    load, small, turn, sent, arrived, few_sent, few_arrived = refs[len(SCRATCH) :]
    p = Place()
    x, y, z = p.at.values()
    all_here = greet(p)
    loads = Loads(p, terms, T, load)
    loads.start(AHEAD)

    def rows_fetch():
        first = (X * Y * PART) * x + 20 * y + lax.div(PART * z, 2)
        for layer in range(LAYERS):
            for w in range(2):
                for i, row in enumerate((lax.max(z - 1, 0), lax.min(z, HIGH - 1))):
                    pltpu.make_async_copy(weights[w].at[layer, x, y, row], s["old"].at[w, layer, i], small.at[0]).start()
            pltpu.make_async_copy(weights[2].at[layer, pl.ds(first, 3)], s["old_down"].at[layer], small.at[1]).start()
        for i in range(2):
            for w in range(2):
                pltpu.make_async_copy(moments[3 * i + w], s["raw"].at[i, w], small.at[2]).start()
            pltpu.make_async_copy(moments[3 * i + 2], s["raw_down"].at[i], small.at[3]).start()

    def rows_here():
        for i, name in enumerate(("old", "old_down", "raw", "raw_down")):
            pltpu.make_async_copy(s[name], s[name], small.at[i]).wait()

    chores, later = [rows_fetch, rows_here], []

    def rows_in(w, layer):
        low, high = (s["old"][w, layer, i].reshape(2 * HALF, *TILE).astype(F32) for i in range(2))
        s["w"][w, layer] = joined(low, high, z)

    def rows_in_low(layer):
        part = [s["old_down"][layer, j].astype(F32) for j in range(3)]
        for j in range(3):
            s["w_low"][layer, j] = jnp.where(lax.rem(z, 2) == 1, joined(part[j], part[min(j + 1, 2)], ROWS // 2), part[j])

    def moments_in(i, w, layer):
        @pl.loop(0, 2 * HALF)
        def _(c):
            s["mv"][i, w, layer, c, pl.ds(0, HIGH)] = s["raw"][i, w, :, layer, lanes(c)]

    def moments_in_low(i, layer):
        @pl.loop(0, HIGH)
        def _(c):
            for j, n in enumerate(DOWN_ROWS):
                s["mv_low"][i, layer, j, c, pl.ds(0, n)] = s["raw_down"][i, pl.ds(ROWS * j, n), layer, lanes(c)]

    def moments_out(i, w, layer):
        @pl.loop(0, 2 * HALF)
        def _(c):
            rows = pl.ds(LAYERS * c + layer, HIGH, stride=LAYERS * 2 * HALF)
            made[3 * i + w][rows, :] = s["mv"][i, w, layer, c, pl.ds(0, HIGH)]

    def moments_out_low(i, layer):
        @pl.loop(0, HIGH)
        def _(c):
            for j, k in enumerate(DOWN_ROWS):
                rows = pl.ds(ROWS * j * LAYERS * HIGH + LAYERS * c + layer, k, stride=LAYERS * HIGH)
                made[3 * i + 2][rows, :] = s["mv_low"][i, layer, j, c, pl.ds(0, k)]

    for layer in range(LAYERS):
        for w in range(2):
            chores.append(functools.partial(rows_in, w, layer))
            for i in range(2):
                chores.append(functools.partial(moments_in, i, w, layer))
                later.append(functools.partial(moments_out, i, w, layer))
        chores.append(functools.partial(rows_in_low, layer))
        for i in range(2):
            chores.append(functools.partial(moments_in_low, i, layer))
            later.append(functools.partial(moments_out_low, i, layer))

    all_here()
    reduce = Reduce(p, T, O, loads, sent, arrived)
    pl.when(p.rep == 0)(lambda: pl.semaphore_wait(turn, 1))
    for n, t in enumerate(REDUCE_ORDER):
        reduce.send(t)
        if n == TURN:
            pl.when(p.rep == 1)(lambda: pl.semaphore_signal(turn, inc=1, device_id=p.twin, device_id_type=MESH))
        if n > len(REDUCE_ORDER) // 4 and n % 4 == 0 and chores:
            chores.pop(0)()

    few = Few(p, few_sent, few_arrived)
    squares = jnp.zeros(TILE, F32)
    for c in COLOURS:
        g = reduce.own(c)
        if c == "B":
            s["own_low"][...] = g
        else:
            s["own"][:, pl.ds(*((0, LEFT) if c == "A" else (LEFT, HALF - LEFT)))] = g
        squares = squares + jnp.sum((g * g).reshape(tiles(c), *TILE), axis=0)
    s["z_sum"][z] = squares
    line_sums = few.tell(s["z_sum"], z, p.line_device[1:])

    for k in range(Z):
        at = s["own"][min(k, HIGH - 1)]
        s["out"][k] = (joined(s["own"][k - 1], at, k) if k else at).astype(BF16)
    pieces = few.line(s["out"], s["into"])
    s["into"][z] = s["out"][z]
    g = [s["own_low"][j] for j in range(PART)]
    for j in range(3):
        s["out_low"][0, j] = g[j].astype(BF16)
        s["out_low"][1, j] = joined(g[2 + j], g[min(3 + j, PART - 1)], ROWS // 2).astype(BF16)
    mine = lax.rem(z, 2)
    other, partner = 1 - mine, p.device(z=z + 1 - 2 * mine)
    pieces_low = few.exchange([(s["out_low"].at[other], s["into_low"].at[mine], partner)], s["into_low"].at[other])
    s["into_low"][mine] = s["out_low"][mine]

    line_sums()
    at = Y * x + y
    s["sum"][at] = jnp.sum(s["z_sum"][...], axis=0)
    sums = few.tell(s["sum"], at, p.plane_device[1:])
    pieces()
    pieces_low()
    sums()
    total = jnp.sum(s["sum"][...], axis=0)
    total = jnp.sum(jnp.sum(total, axis=1, keepdims=True), axis=0, keepdims=True)
    factor = jnp.minimum(1.0, 0.5 * lax.rsqrt(total / COUNT + 1e-30))

    for owner in range(Z):
        w, layer, part = owner // X, owner // 2 % 2, pl.ds(owner % 2 * HALF, HALF)
        g = s["into"][owner].astype(F32) * factor
        new, m, v = adamw(s["w"][w, layer, part], s["mv"][0, w, layer, part], s["mv"][1, w, layer, part], g)
        s["mv"][0, w, layer, part], s["mv"][1, w, layer, part] = m, v
        s["new"][owner] = new.astype(BF16)
    pieces = few.line(s["new"], s["news"])
    for layer in range(LAYERS):
        g = s["into_low"][layer].astype(F32) * factor
        new, m, v = adamw(s["w_low"][layer], s["mv_low"][0, layer], s["mv_low"][1, layer], g)
        s["mv_low"][0, layer], s["mv_low"][1, layer] = m, v
        s["new_low"][layer] = new.astype(BF16)
    pieces_low = few.exchange([(s["new_low"].at[other], s["news_low"].at[mine], partner)], s["news_low"].at[other])
    s["news_low"][mine] = s["new_low"][mine]
    s["news"][z] = s["new"][z]

    own = {c: tuple(p.at[d] for d in DIMS[c]) for c in COLOURS}

    def whole_low():
        pieces_low()
        a, b = ([s["news_low"][i, j].astype(F32) for j in range(3)] for i in range(2))
        seam = jnp.where(rows_of(b[0]) < ROWS // 2, a[2], pltpu.roll(b[0], ROWS // 2, 1))
        for i, tile in enumerate((a[0], a[1], seam, *(joined(b[j], b[j + 1], ROWS // 2) for j in range(2)))):
            O["B"][(*own["B"], i)] = tile.astype(BF16)

    def whole():
        pieces()
        t = [s["news"][k].astype(F32) for k in range(Z)]
        for i in range(HIGH):
            a = pltpu.roll(t[i], ROWS - i, 1) if i else t[i]
            tile = jnp.where(rows_of(a) < HIGH - i, a, pltpu.roll(t[i + 1], HIGH - i, 1)).astype(BF16)
            O["A"][(*own["A"], i)] = tile[:LEFT]
            O["C"][(*own["C"], i)] = tile[LEFT:]

    all_sent(T, sent)
    gather = Gather(p, O, sent, arrived)
    prepare = {"B": whole_low, "A": whole}
    for n, t in enumerate(GATHER_ORDER):
        needs = "B" if t[0] == "B" else "A"
        if needs in prepare:
            prepare.pop(needs)()
        gather.send(t)
        if n > len(GATHER_ORDER) // 4 and n % 4 == 0 and later:
            later.pop(0)()
    for t in GATHER_ENDS:
        gather.wait(t)
    for wait in few.waits:
        wait()
    all_sent(T, sent)


def put(*refs):
    (a, b, c), moments, results, sem = refs[:3], refs[3:9], refs[9:18], refs[18]

    def copy(src, i, *at):
        pltpu.make_async_copy(src, results[i].at[at] if at else results[i], sem.at[i]).start()

    for z in range(Z):
        half, layer = z % 2, z // 2 % 2
        copy(a.at[:, :, z], z // X, layer, slice(None), slice(None), slice(None), half, pl.ds(0, LEFT))
        copy(c.at[z], z // X, layer, slice(None), slice(None), slice(None), half, pl.ds(LEFT, HALF - LEFT))
        layer, q = down_place(z)
        for y in range(Y):
            copy(b.at[y, z], 2, layer, slice(None), y, q)
    for i, moment in enumerate(moments):
        copy(moment, 3 + i)
    for i, ref in enumerate(results):
        pltpu.make_async_copy(ref, ref, sem.at[i]).wait()


def tiled(a, *cut):
    rows, columns = cut
    n = len(rows)
    a = a.reshape(LAYERS, *rows, ROWS, *columns, LANES)
    order = [*range(n + 1), *range(n + 2, n + 2 + len(columns)), n + 1, a.ndim - 1]
    return a.transpose(order)


def untiled(a, *cut):
    rows, columns = cut
    n = len(rows)
    order = [*range(n + 1), a.ndim - 2, *range(n + 1, a.ndim - 2), a.ndim - 1]
    a = a.transpose(order)
    return a.reshape(LAYERS, -1, a.shape[-1] * (HALF * 2 if len(columns) == 2 else HIGH))


WIDE, TALL = ((X, Y, HIGH), (2, HALF)), ((X, Y, X, PART), (HIGH,))


def unmoment(a, rows, columns):
    return a.reshape(rows, columns, LAYERS, LANES).transpose(0, 2, 1, 3).reshape(rows, LAYERS, columns * LANES).transpose(1, 0, 2)


def solution(mesh):
    shapes = [pltpu.VMEM((*lens(c), *BLOCK[c], *TILE), BF16) for c in COLOURS]
    hbm, vmem = pl.BlockSpec(memory_space=pltpu.HBM), pl.BlockSpec(memory_space=pltpu.VMEM)
    moment = (LAYERS * HIGH * HALF * 2, LANES)

    def semaphores(n):
        return pltpu.SemaphoreType.DMA((n,))

    def kernel(body, name, params, **more):
        return pl.pallas_call(body, name=name, compiler_params=pltpu.CompilerParams(**params), **more)

    def step(*arrays):
        terms, weights, moments = [t[0] for t in arrays[:3]], arrays[3:6], arrays[6:]
        wide = [tiled(a, *WIDE) for a in (*terms[:2], *weights[:2])]
        operands = [*wide[:2], tiled(terms[2], *TALL), *wide[2:], tiled(weights[2], (FF // ROWS,), (HIGH,))]
        operands += [a.transpose(1, 0, 2) for a in moments]
        made = kernel(
            work,
            "work",
            dict(collective_id=0, has_side_effects=True, vmem_limit_bytes=34 << 20),
            out_shape=(*shapes, *[pltpu.VMEM(moment, F32)] * 6),
            in_specs=[hbm] * 12,
            out_specs=[vmem] * 9,
            scratch_shapes=[
                *shapes,
                *(pltpu.VMEM(*a) for a in SCRATCH.values()),
                semaphores(AHEAD),
                semaphores(4),
                pltpu.SemaphoreType.REGULAR,
                *(semaphores(n) for n in (len(S_ID), len(R_ID), 6, 6)),
            ],
        )(*(pltpu.with_memory_space_constraint(a, pltpu.HBM) for a in operands))
        out = kernel(
            put,
            "put",
            dict(vmem_limit_bytes=1 << 20),
            out_shape=[jax.ShapeDtypeStruct(a.shape, BF16) for a in operands[:3]] + [jax.ShapeDtypeStruct(moment, F32)] * 6,
            in_specs=[vmem] * 9,
            out_specs=[hbm] * 9,
            scratch_shapes=[semaphores(9)],
        )(*made)
        weights = [untiled(a, *cut) for a, cut in zip(out, (WIDE, WIDE, TALL))]
        return (*weights, *(unmoment(a, *m.shape[1:2], m.shape[2] // LANES) for a, m in zip(out[3:], moments)))

    all_of, cut = P(None, None, None), P(None, "dp", None)
    return jax.shard_map(
        step,
        mesh=mesh,
        in_specs=(P(("rep", "dp"), None, None, None),) * 3 + (all_of,) * 3 + (cut,) * 6,
        out_specs=(P("rep", None, None),) * 3 + (P("rep", "dp", None),) * 6,
        check_vma=False,
    )
```

```python
import functools

import jax
import jax.numpy as jnp
from jax import lax
from jax.experimental import pallas as pl
from jax.experimental.pallas import tpu as pltpu
from jax.sharding import PartitionSpec as P

MESH = pl.DeviceIdType.MESH
F32, BF16 = jnp.float32, jnp.bfloat16
X, Y, Z = 4, 4, 8
SIZE = {"x": X, "y": Y, "z": Z}
DIMS = {"A": ("x", "y", "z"), "B": ("y", "z", "x"), "C": ("z", "x", "y")}
COLOURS = tuple(DIMS)
LAYERS, ROWS, LANES = 2, 8, 128
TILE = (ROWS, LANES)
D, FF = 896, 2560
HIGH, HALF, LEFT, PART = 7, 10, 6, 5
BLOCK = {"A": (HIGH, LEFT), "B": (PART, HIGH), "C": (HIGH, HALF - LEFT)}
COUNT = 3 * LAYERS * D * FF


def lens(c):
    return tuple(SIZE[d] for d in DIMS[c])


def tiles(c):
    return BLOCK[c][0] * BLOCK[c][1]


def down_place(z):
    return z % 2, z // 2


def ring(n, ant):
    return [(ant, n // 2)] + [(d, k) for k in range(n // 2 - 1, 0, -1) for d in (1, -1)]


def slots(n, ant):
    return {m: i for i, m in enumerate(sorted(ring(n, ant), key=lambda m: (m[1], -m[0])))}


def far_first(n):
    return [n // 2] + [s * k for k in range(n // 2 - 1, 0, -1) for s in (1, -1)] + [0]


def ant_of(o):
    return -1 if o % 2 else 1


def ant_in(phase, unit):
    return (1, ant_of(sum(o for o in unit if o is not None)) if unit else 1)[phase < 3]


def came(c, phase, unit, n, o):
    far = n - o < n // 2 or (n == 2 * o and ant_in(phase, unit) == 1)
    return (c, phase, unit, 1, n - o) if far else (c, phase, unit, -1, o)


SECOND_BY_BLOCK, FIRST_BY_BLOCK = "AC", "A"


def gather_messages():
    out = {}
    for c in COLOURS:
        n1, n2, n3 = lens(c)

        def add(phase, unit, count, first):
            dim = DIMS[c][phase - 1]
            for d, k in ring(SIZE[dim], ant_in(phase, unit)):
                out[c, phase, unit, d, k] = ((dim, d), count * tiles(c), [(c, phase, unit, d, k - 1)] if k > 1 else first)

        blocks, whole = [(o,) for o in range(n3)], [(None,)]
        add(3, (), 1, [])
        line = [came(c, 3, (), n3, o) for o in range(1, n3)]
        second = blocks if c in SECOND_BY_BLOCK else whole
        for phase, head, chosen in ((2, (), second), (1, (0,), blocks if c in FIRST_BY_BLOCK else whole)):
            for unit in chosen:
                add(phase, head + unit, 1 if unit[0] is not None else n3, line[unit[0] - 1 : unit[0]] if unit[0] is not None else line)
        for o in range(1, n2):
            add(1, (o, None), n3, [came(c, 2, unit, n2, o) for unit in second])
    return out


def ordered(messages, slack, latency, rate):
    users, tail = {t: [] for t in messages}, {}
    for t, (_, _, waits) in messages.items():
        for w in waits:
            users[w].append(t)

    def way(t):
        if t not in tail:
            tail[t] = 2 * messages[t][1] / rate + latency + max((way(u) for u in users[t]), default=0)
        return tail[t]

    for t in messages:
        way(t)
    queues = {m[0]: [] for m in messages.values()}
    left, arrives, now, starts = list(messages), {}, 0.0, []
    while left or any(queues.values()):
        ready = [
            t
            for t in left
            if all(arrives.get(w, now + 1) <= now for w in messages[t][2])
            and 2 * sum(q[1] for q in queues[messages[t][0]]) <= slack
        ]
        if ready:
            t = max(ready, key=way)
            left.remove(t)
            starts.append(t)
            queues[messages[t][0]].append([t, messages[t][1] / rate])
            continue
        speed = {(m, d): 1 / 2 if queues[m, -d] else 1 for (m, d), q in queues.items() if q}
        full = {link: sum(q[1] for q in queues[link]) - slack / 2 for link in speed}
        events = [queues[link][0][1] / s for link, s in speed.items()] + [full[link] / s for link, s in speed.items() if full[link] > 0]
        pause = min(events + [a - now for a in arrives.values() if a > now]) + 1e-6
        now += pause
        for link, s in speed.items():
            queues[link][0][1] -= pause * s
            if queues[link][0][1] <= 0:
                arrives[queues[link].pop(0)[0]] = now + latency
    return starts, list(arrives)


GATHER = gather_messages()
GATHER_ORDER, GATHER_ENDS = ordered(GATHER, 5.0, 2.0, 43.0)
ENDS = ordered(GATHER, 4.0, 1.0, 50.0)[1]
TURN = 59
AHEAD = 8


def back(t):
    c, phase, unit, d, k = t
    return (c, phase, unit, -d, k)


REDUCE = {back(t): (link, n, []) for t, (link, n, _) in GATHER.items()}
for t, (_, _, waits) in GATHER.items():
    for w in waits:
        REDUCE[back(w)][2].append(back(t))
REDUCE_ORDER = [back(t) for t in reversed(ENDS)]
R_ID = {t: i for i, t in enumerate(REDUCE)}
G_ID = {t: R_ID[back(t)] for t in GATHER}
S_ID = {t: i for i, t in enumerate((c, phase) for c in COLOURS for phase in range(1, 4))}


def all_sent(T, sem):
    for (c, phase), i in S_ID.items():
        n = lens(c)[phase - 1] - 1
        ref = T[c].at[(*[0] * (phase - 1), pl.ds(0, n))]
        pltpu.make_async_copy(ref, ref, sem.at[i]).wait()


class Place:
    def __init__(self):
        dp = lax.axis_index("dp")
        rep = lax.axis_index("rep")
        self.at = at = {"x": lax.div(dp, Y * Z), "y": lax.rem(lax.div(dp, Z), Y), "z": lax.rem(dp, Z)}
        sign = 1 - 2 * rep
        self.offset = {(d, k): lax.rem(at[d] + sign * k + n, n) for d, n in SIZE.items() for k in range(-n // 2, n // 2) if k}

        def device(**moved):
            a = {**at, **moved}
            return (rep, (a["x"] * Y + a["y"]) * Z + a["z"])

        def ahead(d, k):
            return lax.rem(at[d] + SIZE[d] + k, SIZE[d])

        self.rep, self.device, self.twin = rep, device, (1 - rep, dp)
        self.beside = {(d, e): device(**{d: self.offset[d, e]}) for d in SIZE for e in (1, -1)}
        self.line = [ahead("z", k) for k in range(Z)]
        self.line_device = [device(z=to) for to in self.line]
        self.plane_device = [device(x=ahead("x", k // Y), y=ahead("y", k % Y)) for k in range(X * Y)]

    def off(self, dim, k):
        n = SIZE[dim]
        k = (k + n // 2) % n - n // 2
        return self.offset[dim, k] if k else self.at[dim]


def greet(p):
    peers = [*p.beside.values(), p.twin]
    barrier = pltpu.get_barrier_semaphore()
    for peer in peers:
        pl.semaphore_signal(barrier, inc=1, device_id=peer, device_id_type=MESH)
    return lambda: pl.semaphore_wait(barrier, len(peers))


def block_of(t):
    c, phase, unit, d, k = t
    n1, n2, _ = lens(c)
    return (c, d * k % n1, unit[0] % n2) if phase == 1 else (c, 0, d * k % n2 if phase == 2 else 0)


class Loads:
    def __init__(self, p, terms, T, sem):
        self.p, self.terms, self.T, self.sem = p, terms, T, sem
        self.left = list(dict.fromkeys([block_of(t) for t in REDUCE_ORDER] + [(c, 0, 0) for c in COLOURS]))
        self.place = {part: i % AHEAD for i, part in enumerate(self.left)}

    def at(self, part):
        c, k, o = part
        return self.p.off(DIMS[c][0], k), self.p.off(DIMS[c][1], o)

    def start(self, count):
        gate, up, down = self.terms
        for part in self.left[:count]:
            c, (i, j), s = part[0], self.at(part), self.sem.at[self.place[part]]
            T = self.T[c].at[i, j]
            if c == "A":
                for z in range(Z):
                    src = (gate, up)[z // X].at[z // 2 % 2, i, j, :, z % 2, pl.ds(0, LEFT)]
                    pltpu.make_async_copy(src, T.at[z], s).start()
            elif c == "B":
                pltpu.make_async_copy(down.at[lax.rem(j, 2), :, i, lax.div(j, 2)], T, s).start()
            else:
                layer, half = lax.rem(lax.div(i, 2), 2), lax.rem(i, 2)

                def load(ref):
                    pltpu.make_async_copy(ref.at[layer, j, :, :, half, pl.ds(LEFT, HALF - LEFT)], T, s).start()

                pl.when(i < X)(lambda: load(gate))
                pl.when(i >= X)(lambda: load(up))
        self.left = self.left[count:]

    def wait(self, part):
        if part in self.place:
            ref = self.T[part[0]].at[self.at(part)]
            pltpu.make_async_copy(ref, ref, self.sem.at[self.place.pop(part)]).wait()
            self.start(1)


class Reduce:
    def __init__(self, p, T, O, load, sent, arrived):
        self.p, self.T, self.O, self.load, self.sent, self.arrived = p, T, O, load, sent, arrived
        self.waited = set()


    def areas(self, t):
        c, phase, unit, d, k = t
        n1, n2, n3 = lens(c)
        d1, d2, d3 = DIMS[c]
        p = self.p
        slot = slots(SIZE[DIMS[c][phase - 1]], -ant_in(phase, unit))[d, k]
        if phase == 1:
            j2 = p.off(d2, unit[0])
            first, count = (0, n3) if unit[1] is None else (p.off(d3, unit[1]), 1)
            return (p.off(d1, d * k), j2), first, (slot, j2), first, count
        if phase == 2:
            first, count = (0, n3) if unit[0] is None else (p.off(d3, unit[0]), 1)
            return (p.at[d1], p.off(d2, d * k)), first, (n1 - 1, slot), first, count
        return (p.at[d1], p.at[d2]), p.off(d3, d * k), (n1 - 1, n2 - 1), slot, 1

    def copy(self, t):
        c, phase, _, d, _ = t
        src, i, dst, j, n = self.areas(t)
        s = R_ID[t]
        return pltpu.make_async_remote_copy(
            src_ref=self.T[c].at[(*src, pl.ds(i, n))],
            dst_ref=self.O[c].at[(*dst, pl.ds(j, n))],
            send_sem=self.sent.at[S_ID[c, phase]],
            recv_sem=self.arrived.at[s],
            device_id=self.p.beside[DIMS[c][phase - 1], d],
            device_id_type=MESH,
        )

    def wait(self, t):
        if t not in self.waited:
            self.waited.add(t)
            self.copy(t).wait_recv()

    def ended(self, c, phase, j2, j3):
        last = lens(c)[0] - 1
        return [(0, j2, j3), (1, j2, j3), (last, 0, j3), (last, 1, j3)][: 2 * (phase - 1)]

    def send(self, t):
        c, phase, unit, d, k = t
        T, O = self.T[c], self.O[c]
        for w in REDUCE[t][2]:
            self.wait(w)
        self.load.wait(block_of(t))
        src, first, _, _, count = self.areas(t)
        before = (c, phase, unit, d, k + 1)
        chain = before in R_ID
        if phase > 1 or chain:
            _, _, there, start, _ = self.areas(before if chain else t)

            def one(i):
                parts = self.ended(c, phase, src[1], first + i)
                if chain:
                    parts.append((*there, start + i))
                total = T[(*src, first + i)].astype(F32)
                for part in parts:
                    total = total + O[part].astype(F32)
                T[(*src, first + i)] = total.astype(BF16)

            if count == 1:
                one(0)
            else:
                pl.loop(0, count)(one)
        self.copy(t).start()

    def own(self, c):
        n1, n2, _ = lens(c)
        for t in REDUCE:
            if t[0] == c and t[-1] == 1 and not any(t[2]):
                self.wait(t)
        self.load.wait((c, 0, 0))
        i, j, k = (self.p.at[d] for d in DIMS[c])
        total = self.T[c][i, j, k].astype(F32)
        for part in self.ended(c, 3, j, k) + [(n1 - 1, n2 - 1, e) for e in (0, 1)]:
            total = total + self.O[c][part].astype(F32)
        return total.astype(BF16).astype(F32)


class Gather:
    def __init__(self, p, O, sent, arrived):
        self.p, self.O, self.sent, self.arrived = p, O, sent, arrived
        self.waited = set()

    def copy(self, t, came=0):
        c, phase, unit, d, k = t
        d1, d2, d3 = DIMS[c]
        p, dim = self.p, DIMS[c][phase - 1]
        behind = p.off(dim, d * (1 - came - k))
        at = (behind, p.off(d2, unit[0])) if phase == 1 else (p.at[d1], behind) if phase == 2 else (p.at[d1], p.at[d2], behind)
        at += tuple(p.off(d3, o) for o in unit[-1:] if o is not None)
        ref, s = self.O[c].at[at], G_ID[t]
        return pltpu.make_async_remote_copy(
            src_ref=ref,
            dst_ref=ref,
            send_sem=self.sent.at[S_ID[c, phase]],
            recv_sem=self.arrived.at[s],
            device_id=p.beside[dim, d],
            device_id_type=MESH,
        )

    def wait(self, t):
        if t not in self.waited:
            self.waited.add(t)
            self.copy(t, 1).wait_recv()

    def send(self, t):
        for w in GATHER[t][2]:
            self.wait(w)
        self.copy(t).start()


def rows_of(a):
    return lax.broadcasted_iota(jnp.int32, a.shape, a.ndim - 2)


def joined(a, b, k):
    return pltpu.roll(jnp.where(rows_of(b) >= ROWS - k, a, b), k, b.ndim - 2)


def adamw(w, m, v, g):
    m = 0.9 * m + 0.1 * g
    v = 0.95 * v + 0.05 * g * g
    return w - 0.02 * (m * lax.rsqrt(v + 1e-8) + 0.1 * w), m, v


DOWN_ROWS = (ROWS, ROWS, ROWS // 2)
SCRATCH = {
    "raw": ((2, 2, HIGH, LAYERS, FF), F32),
    "raw_down": ((2, 20, LAYERS, D), F32),
    "own": ((HIGH, HALF, *TILE), F32),
    "own_low": ((PART, HIGH, *TILE), F32),
    "old": ((2, LAYERS, 2, 2, HALF, *TILE), BF16),
    "old_down": ((LAYERS, 3, HIGH, *TILE), BF16),
    "w": ((2, LAYERS, 2 * HALF, *TILE), F32),
    "w_low": ((LAYERS, 3, HIGH, *TILE), F32),
    "mv": ((2, 2, LAYERS, 2 * HALF, *TILE), F32),
    "mv_low": ((2, LAYERS, 3, HIGH, *TILE), F32),
    "out": ((Z, HALF, *TILE), BF16),
    "into": ((Z, HALF, *TILE), BF16),
    "out_low": ((2, 3, HIGH, *TILE), BF16),
    "into_low": ((LAYERS, 3, HIGH, *TILE), BF16),
    "new": ((Z, HALF, *TILE), BF16),
    "news": ((Z, HALF, *TILE), BF16),
    "new_low": ((LAYERS, 3, HIGH, *TILE), BF16),
    "news_low": ((2, 3, HIGH, *TILE), BF16),
    "z_sum": ((Z, 1, LANES), F32),
    "sum": ((X * Y, 1, LANES), F32),
}


class Few:
    def __init__(self, p, sent, arrived):
        self.p, self.sent, self.arrived, self.waits = p, sent, arrived, []

    def exchange(self, copies, get):
        i = len(self.waits)
        for src, dst, to in copies:
            one = pltpu.make_async_remote_copy(
                src_ref=src, dst_ref=dst, send_sem=self.sent.at[i], recv_sem=self.arrived.at[i], device_id=to, device_id_type=MESH
            )
            one.start()
        self.waits.append(pltpu.make_async_copy(get, get, self.sent.at[i]).wait)
        return pltpu.make_async_copy(get, get, self.arrived.at[i]).wait

    def line(self, out, into, make):
        p, i = self.p, len(self.waits)
        z, get = p.at["z"], into.at[pl.ds(0, Z - 1)]
        for k in range(Z):
            make(k)

            @pl.when(z != k)
            def _():
                pltpu.make_async_remote_copy(
                    src_ref=out.at[k],
                    dst_ref=into.at[z],
                    send_sem=self.sent.at[i],
                    recv_sem=self.arrived.at[i],
                    device_id=p.device(z=k),
                    device_id_type=MESH,
                ).start()

        into[z] = out[z]
        self.waits.append(pltpu.make_async_copy(get, get, self.sent.at[i]).wait)
        return pltpu.make_async_copy(get, get, self.arrived.at[i]).wait

    def tell(self, ref, at, devices):
        return self.exchange([(ref.at[at], ref.at[at], to) for to in devices], ref.at[pl.ds(0, len(devices))])


def lanes(c):
    return pl.ds(pl.multiple_of(c * LANES, LANES), LANES)


def work(*refs):
    terms, weights, moments, refs = refs[:3], refs[3:6], refs[6:12], refs[12:]
    outs, made, refs = refs[:3], refs[3:9], refs[9:]
    O, T, refs = dict(zip(COLOURS, outs)), dict(zip(COLOURS, refs)), refs[3:]
    s = dict(zip(SCRATCH, refs))
    load, small, turn, sent, arrived, few_sent, few_arrived = refs[len(SCRATCH) :]
    p = Place()
    x, y, z = p.at.values()
    all_here = greet(p)
    loads = Loads(p, terms, T, load)
    loads.start(AHEAD)

    def rows_fetch():
        first = (X * Y * PART) * x + 20 * y + lax.div(PART * z, 2)
        for layer in range(LAYERS):
            for w in range(2):
                for i, row in enumerate((lax.max(z - 1, 0), lax.min(z, HIGH - 1))):
                    pltpu.make_async_copy(weights[w].at[layer, x, y, row], s["old"].at[w, layer, i], small.at[0]).start()
            pltpu.make_async_copy(weights[2].at[layer, pl.ds(first, 3)], s["old_down"].at[layer], small.at[1]).start()
        for i in range(2):
            for w in range(2):
                pltpu.make_async_copy(moments[3 * i + w], s["raw"].at[i, w], small.at[2]).start()
            pltpu.make_async_copy(moments[3 * i + 2], s["raw_down"].at[i], small.at[3]).start()

    def rows_here():
        for i, name in enumerate(("old", "old_down", "raw", "raw_down")):
            pltpu.make_async_copy(s[name], s[name], small.at[i]).wait()

    chores, later = [rows_fetch, rows_here], []

    def rows_in(w, layer):
        low, high = (s["old"][w, layer, i].reshape(2 * HALF, *TILE).astype(F32) for i in range(2))
        s["w"][w, layer] = joined(low, high, z)

    def rows_in_low(layer):
        part = [s["old_down"][layer, j].astype(F32) for j in range(3)]
        for j in range(3):
            s["w_low"][layer, j] = jnp.where(lax.rem(z, 2) == 1, joined(part[j], part[min(j + 1, 2)], ROWS // 2), part[j])

    def moments_in(i, w, layer):
        @pl.loop(0, 2 * HALF)
        def _(c):
            s["mv"][i, w, layer, c, pl.ds(0, HIGH)] = s["raw"][i, w, :, layer, lanes(c)]

    def moments_in_low(i, layer):
        @pl.loop(0, HIGH)
        def _(c):
            for j, n in enumerate(DOWN_ROWS):
                s["mv_low"][i, layer, j, c, pl.ds(0, n)] = s["raw_down"][i, pl.ds(ROWS * j, n), layer, lanes(c)]

    def moments_out(i, w, layer):
        @pl.loop(0, 2 * HALF)
        def _(c):
            rows = pl.ds(LAYERS * c + layer, HIGH, stride=LAYERS * 2 * HALF)
            made[3 * i + w][rows, :] = s["mv"][i, w, layer, c, pl.ds(0, HIGH)]

    def moments_out_low(i, layer):
        @pl.loop(0, HIGH)
        def _(c):
            for j, k in enumerate(DOWN_ROWS):
                rows = pl.ds(ROWS * j * LAYERS * HIGH + LAYERS * c + layer, k, stride=LAYERS * HIGH)
                made[3 * i + 2][rows, :] = s["mv_low"][i, layer, j, c, pl.ds(0, k)]

    for layer in range(LAYERS):
        for w in range(2):
            chores.append(functools.partial(rows_in, w, layer))
            for i in range(2):
                chores.append(functools.partial(moments_in, i, w, layer))
                later.append(functools.partial(moments_out, i, w, layer))
        chores.append(functools.partial(rows_in_low, layer))
        for i in range(2):
            chores.append(functools.partial(moments_in_low, i, layer))
            later.append(functools.partial(moments_out_low, i, layer))

    all_here()
    reduce = Reduce(p, T, O, loads, sent, arrived)
    pl.when(p.rep == 0)(lambda: pl.semaphore_wait(turn, 1))
    for n, t in enumerate(REDUCE_ORDER):
        reduce.send(t)
        if n == TURN:
            pl.when(p.rep == 1)(lambda: pl.semaphore_signal(turn, inc=1, device_id=p.twin, device_id_type=MESH))
        if n > len(REDUCE_ORDER) // 4 and n % 4 == 0 and chores:
            chores.pop(0)()

    few = Few(p, few_sent, few_arrived)
    squares = jnp.zeros(TILE, F32)
    for c in COLOURS:
        g = reduce.own(c)
        if c == "B":
            s["own_low"][...] = g
        else:
            s["own"][:, pl.ds(*((0, LEFT) if c == "A" else (LEFT, HALF - LEFT)))] = g
        squares = squares + jnp.sum((g * g).reshape(tiles(c), *TILE), axis=0)
    s["z_sum"][z] = jnp.sum(squares, axis=0, keepdims=True)
    line_sums = few.tell(s["z_sum"], z, p.line_device[1:])

    def piece(k):
        at = s["own"][min(k, HIGH - 1)]
        s["out"][k] = (joined(s["own"][k - 1], at, k) if k else at).astype(BF16)

    pieces = few.line(s["out"], s["into"], piece)
    g = [s["own_low"][j] for j in range(PART)]
    for j in range(3):
        s["out_low"][0, j] = g[j].astype(BF16)
        s["out_low"][1, j] = joined(g[2 + j], g[min(3 + j, PART - 1)], ROWS // 2).astype(BF16)
    mine = lax.rem(z, 2)
    other, partner = 1 - mine, p.device(z=z + 1 - 2 * mine)
    pieces_low = few.exchange([(s["out_low"].at[other], s["into_low"].at[mine], partner)], s["into_low"].at[other])
    s["into_low"][mine] = s["out_low"][mine]

    line_sums()
    at = Y * x + y
    s["sum"][at] = jnp.sum(s["z_sum"][...], axis=0)
    sums = few.tell(s["sum"], at, p.plane_device[1:])
    pieces()
    pieces_low()
    sums()
    total = jnp.sum(jnp.sum(s["sum"][...], axis=0), axis=1, keepdims=True)
    factor = jnp.minimum(1.0, 0.5 * lax.rsqrt(total / COUNT + 1e-30))

    def step(owner):
        w, layer, part = owner // X, owner // 2 % 2, pl.ds(owner % 2 * HALF, HALF)
        g = s["into"][owner].astype(F32) * factor
        new, m, v = adamw(s["w"][w, layer, part], s["mv"][0, w, layer, part], s["mv"][1, w, layer, part], g)
        s["mv"][0, w, layer, part], s["mv"][1, w, layer, part] = m, v
        s["new"][owner] = new.astype(BF16)

    pieces = few.line(s["new"], s["news"], step)
    for layer in range(LAYERS):
        g = s["into_low"][layer].astype(F32) * factor
        new, m, v = adamw(s["w_low"][layer], s["mv_low"][0, layer], s["mv_low"][1, layer], g)
        s["mv_low"][0, layer], s["mv_low"][1, layer] = m, v
        s["new_low"][layer] = new.astype(BF16)
    pieces_low = few.exchange([(s["new_low"].at[other], s["news_low"].at[mine], partner)], s["news_low"].at[other])
    s["news_low"][mine] = s["new_low"][mine]

    own = {c: tuple(p.at[d] for d in DIMS[c]) for c in COLOURS}

    def whole_low():
        pieces_low()
        a, b = ([s["news_low"][i, j].astype(F32) for j in range(3)] for i in range(2))
        seam = jnp.where(rows_of(b[0]) < ROWS // 2, a[2], pltpu.roll(b[0], ROWS // 2, 1))
        for i, tile in enumerate((a[0], a[1], seam, *(joined(b[j], b[j + 1], ROWS // 2) for j in range(2)))):
            O["B"][(*own["B"], i)] = tile.astype(BF16)

    def whole():
        pieces()
        t = [s["news"][k].astype(F32) for k in range(Z)]
        for i in range(HIGH):
            a = pltpu.roll(t[i], ROWS - i, 1) if i else t[i]
            tile = jnp.where(rows_of(a) < HIGH - i, a, pltpu.roll(t[i + 1], HIGH - i, 1)).astype(BF16)
            O["A"][(*own["A"], i)] = tile[:LEFT]
            O["C"][(*own["C"], i)] = tile[LEFT:]

    all_sent(T, sent)
    gather = Gather(p, O, sent, arrived)
    prepare = {"B": whole_low, "A": whole}
    for n, t in enumerate(GATHER_ORDER):
        needs = "B" if t[0] == "B" else "A"
        if needs in prepare:
            prepare.pop(needs)()
        gather.send(t)
        if n > len(GATHER_ORDER) // 4 and n % 4 == 0 and later:
            later.pop(0)()
    for t in GATHER_ENDS:
        gather.wait(t)
    for wait in few.waits:
        wait()
    all_sent(T, sent)


def put(*refs):
    (a, b, c), moments, results, sem = refs[:3], refs[3:9], refs[9:18], refs[18]

    def copy(src, i, *at):
        pltpu.make_async_copy(src, results[i].at[at] if at else results[i], sem.at[i]).start()

    for z in range(Z):
        half, layer = z % 2, z // 2 % 2
        copy(a.at[:, :, z], z // X, layer, slice(None), slice(None), slice(None), half, pl.ds(0, LEFT))
        copy(c.at[z], z // X, layer, slice(None), slice(None), slice(None), half, pl.ds(LEFT, HALF - LEFT))
        layer, q = down_place(z)
        for y in range(Y):
            copy(b.at[y, z], 2, layer, slice(None), y, q)
    for i, moment in enumerate(moments):
        copy(moment, 3 + i)
    for i, ref in enumerate(results):
        pltpu.make_async_copy(ref, ref, sem.at[i]).wait()


def tiled(a, *cut):
    rows, columns = cut
    n = len(rows)
    a = a.reshape(LAYERS, *rows, ROWS, *columns, LANES)
    order = [*range(n + 1), *range(n + 2, n + 2 + len(columns)), n + 1, a.ndim - 1]
    return a.transpose(order)


def untiled(a, *cut):
    rows, columns = cut
    n = len(rows)
    order = [*range(n + 1), a.ndim - 2, *range(n + 1, a.ndim - 2), a.ndim - 1]
    a = a.transpose(order)
    return a.reshape(LAYERS, -1, a.shape[-1] * (HALF * 2 if len(columns) == 2 else HIGH))


WIDE, TALL = ((X, Y, HIGH), (2, HALF)), ((X, Y, X, PART), (HIGH,))


def unmoment(a, rows, columns):
    return a.reshape(rows, columns, LAYERS, LANES).transpose(0, 2, 1, 3).reshape(rows, LAYERS, columns * LANES).transpose(1, 0, 2)


def solution(mesh):
    shapes = [pltpu.VMEM((*lens(c), *BLOCK[c], *TILE), BF16) for c in COLOURS]
    hbm, vmem = pl.BlockSpec(memory_space=pltpu.HBM), pl.BlockSpec(memory_space=pltpu.VMEM)
    moment = (LAYERS * HIGH * HALF * 2, LANES)

    def semaphores(n):
        return pltpu.SemaphoreType.DMA((n,))

    def kernel(body, name, params, **more):
        return pl.pallas_call(body, name=name, compiler_params=pltpu.CompilerParams(**params), **more)

    def step(*arrays):
        terms, weights, moments = [t[0] for t in arrays[:3]], arrays[3:6], arrays[6:]
        wide = [tiled(a, *WIDE) for a in (*terms[:2], *weights[:2])]
        operands = [*wide[:2], tiled(terms[2], *TALL), *wide[2:], tiled(weights[2], (FF // ROWS,), (HIGH,))]
        operands += [a.transpose(1, 0, 2) for a in moments]
        made = kernel(
            work,
            "work",
            dict(collective_id=0, has_side_effects=True, vmem_limit_bytes=34 << 20),
            out_shape=(*shapes, *[pltpu.VMEM(moment, F32)] * 6),
            in_specs=[hbm] * 12,
            out_specs=[vmem] * 9,
            scratch_shapes=[
                *shapes,
                *(pltpu.VMEM(*a) for a in SCRATCH.values()),
                semaphores(AHEAD),
                semaphores(4),
                pltpu.SemaphoreType.REGULAR,
                *(semaphores(n) for n in (len(S_ID), len(R_ID), 6, 6)),
            ],
        )(*(pltpu.with_memory_space_constraint(a, pltpu.HBM) for a in operands))
        out = kernel(
            put,
            "put",
            dict(vmem_limit_bytes=1 << 20),
            out_shape=[jax.ShapeDtypeStruct(a.shape, BF16) for a in operands[:3]] + [jax.ShapeDtypeStruct(moment, F32)] * 6,
            in_specs=[vmem] * 9,
            out_specs=[hbm] * 9,
            scratch_shapes=[semaphores(9)],
        )(*made)
        weights = [untiled(a, *cut) for a, cut in zip(out, (WIDE, WIDE, TALL))]
        return (*weights, *(unmoment(a, *m.shape[1:2], m.shape[2] // LANES) for a, m in zip(out[3:], moments)))

    all_of, cut = P(None, None, None), P(None, "dp", None)
    return jax.shard_map(
        step,
        mesh=mesh,
        in_specs=(P(("rep", "dp"), None, None, None),) * 3 + (all_of,) * 3 + (cut,) * 6,
        out_specs=(P("rep", None, None),) * 3 + (P("rep", "dp", None),) * 6,
        check_vma=False,
    )
```

```python
import functools

import jax
import jax.numpy as jnp
from jax import lax
from jax.experimental import pallas as pl
from jax.experimental.pallas import tpu as pltpu
from jax.sharding import PartitionSpec as P

MESH = pl.DeviceIdType.MESH
F32, BF16 = jnp.float32, jnp.bfloat16
X, Y, Z = 4, 4, 8
SIZE = {"x": X, "y": Y, "z": Z}
DIMS = {"A": ("x", "y", "z"), "B": ("y", "z", "x"), "C": ("z", "x", "y")}
COLOURS = tuple(DIMS)
LAYERS, ROWS, LANES = 2, 8, 128
TILE = (ROWS, LANES)
D, FF = 896, 2560
HIGH, HALF, LEFT, PART = 7, 10, 6, 5
BLOCK = {"A": (HIGH, LEFT), "B": (PART, HIGH), "C": (HIGH, HALF - LEFT)}
COUNT = 3 * LAYERS * D * FF


def lens(c):
    return tuple(SIZE[d] for d in DIMS[c])


def tiles(c):
    return BLOCK[c][0] * BLOCK[c][1]


def down_place(z):
    return z % 2, z // 2


def ring(n, ant):
    return [(ant, n // 2)] + [(d, k) for k in range(n // 2 - 1, 0, -1) for d in (1, -1)]


def slots(n, ant):
    return {m: i for i, m in enumerate(sorted(ring(n, ant), key=lambda m: (m[1], -m[0])))}


def far_first(n):
    return [n // 2] + [s * k for k in range(n // 2 - 1, 0, -1) for s in (1, -1)] + [0]


def ant_of(o):
    return -1 if o % 2 else 1


def ant_in(phase, unit):
    return (1, ant_of(sum(o for o in unit if o is not None)) if unit else 1)[phase < 3]


def came(c, phase, unit, n, o):
    far = n - o < n // 2 or (n == 2 * o and ant_in(phase, unit) == 1)
    return (c, phase, unit, 1, n - o) if far else (c, phase, unit, -1, o)


SECOND_BY_BLOCK, FIRST_BY_BLOCK = "AC", "A"


def gather_messages():
    out = {}
    for c in COLOURS:
        n1, n2, n3 = lens(c)

        def add(phase, unit, count, first):
            dim = DIMS[c][phase - 1]
            for d, k in ring(SIZE[dim], ant_in(phase, unit)):
                out[c, phase, unit, d, k] = ((dim, d), count * tiles(c), [(c, phase, unit, d, k - 1)] if k > 1 else first)

        blocks, whole = [(o,) for o in range(n3)], [(None,)]
        add(3, (), 1, [])
        line = [came(c, 3, (), n3, o) for o in range(1, n3)]
        second = blocks if c in SECOND_BY_BLOCK else whole
        for phase, head, chosen in ((2, (), second), (1, (0,), blocks if c in FIRST_BY_BLOCK else whole)):
            for unit in chosen:
                add(phase, head + unit, 1 if unit[0] is not None else n3, line[unit[0] - 1 : unit[0]] if unit[0] is not None else line)
        for o in range(1, n2):
            add(1, (o, None), n3, [came(c, 2, unit, n2, o) for unit in second])
    return out


def ordered(messages, slack, latency, rate):
    users, tail = {t: [] for t in messages}, {}
    for t, (_, _, waits) in messages.items():
        for w in waits:
            users[w].append(t)

    def way(t):
        if t not in tail:
            tail[t] = 2 * messages[t][1] / rate + latency + max((way(u) for u in users[t]), default=0)
        return tail[t]

    for t in messages:
        way(t)
    queues = {m[0]: [] for m in messages.values()}
    left, arrives, now, starts = list(messages), {}, 0.0, []
    while left or any(queues.values()):
        ready = [
            t
            for t in left
            if all(arrives.get(w, now + 1) <= now for w in messages[t][2])
            and 2 * sum(q[1] for q in queues[messages[t][0]]) <= slack
        ]
        if ready:
            t = max(ready, key=way)
            left.remove(t)
            starts.append(t)
            queues[messages[t][0]].append([t, messages[t][1] / rate])
            continue
        speed = {(m, d): 1 / 2 if queues[m, -d] else 1 for (m, d), q in queues.items() if q}
        full = {link: sum(q[1] for q in queues[link]) - slack / 2 for link in speed}
        events = [queues[link][0][1] / s for link, s in speed.items()] + [full[link] / s for link, s in speed.items() if full[link] > 0]
        pause = min(events + [a - now for a in arrives.values() if a > now]) + 1e-6
        now += pause
        for link, s in speed.items():
            queues[link][0][1] -= pause * s
            if queues[link][0][1] <= 0:
                arrives[queues[link].pop(0)[0]] = now + latency
    return starts, list(arrives)


GATHER = gather_messages()
GATHER_ORDER, GATHER_ENDS = ordered(GATHER, 5.0, 2.0, 43.0)
ENDS = ordered(GATHER, 4.0, 1.0, 50.0)[1]
TURN = 59
AHEAD = 6


def back(t):
    c, phase, unit, d, k = t
    return (c, phase, unit, -d, k)


REDUCE = {back(t): (link, n, []) for t, (link, n, _) in GATHER.items()}
for t, (_, _, waits) in GATHER.items():
    for w in waits:
        REDUCE[back(w)][2].append(back(t))
REDUCE_ORDER = [back(t) for t in reversed(ENDS)]
R_ID = {t: i for i, t in enumerate(REDUCE)}
G_ID = {t: R_ID[back(t)] for t in GATHER}
S_ID = {t: i for i, t in enumerate((c, phase) for c in COLOURS for phase in range(1, 4))}


def all_sent(T, sem):
    for (c, phase), i in S_ID.items():
        n = lens(c)[phase - 1] - 1
        ref = T[c].at[(*[0] * (phase - 1), pl.ds(0, n))]
        pltpu.make_async_copy(ref, ref, sem.at[i]).wait()


class Place:
    def __init__(self):
        dp = lax.axis_index("dp")
        rep = lax.axis_index("rep")
        self.at = at = {"x": lax.div(dp, Y * Z), "y": lax.rem(lax.div(dp, Z), Y), "z": lax.rem(dp, Z)}
        sign = 1 - 2 * rep
        self.offset = {(d, k): lax.rem(at[d] + sign * k + n, n) for d, n in SIZE.items() for k in range(-n // 2, n // 2) if k}

        def device(**moved):
            a = {**at, **moved}
            return (rep, (a["x"] * Y + a["y"]) * Z + a["z"])

        def ahead(d, k):
            return lax.rem(at[d] + SIZE[d] + k, SIZE[d])

        self.rep, self.device, self.twin = rep, device, (1 - rep, dp)
        self.beside = {(d, e): device(**{d: self.offset[d, e]}) for d in SIZE for e in (1, -1)}
        self.line = [ahead("z", k) for k in range(Z)]
        self.line_device = [device(z=to) for to in self.line]
        self.plane_device = [device(x=ahead("x", k // Y), y=ahead("y", k % Y)) for k in range(X * Y)]

    def off(self, dim, k):
        n = SIZE[dim]
        k = (k + n // 2) % n - n // 2
        return self.offset[dim, k] if k else self.at[dim]


def greet(p):
    peers = [*p.beside.values(), p.twin]
    barrier = pltpu.get_barrier_semaphore()
    for peer in peers:
        pl.semaphore_signal(barrier, inc=1, device_id=peer, device_id_type=MESH)
    return lambda: pl.semaphore_wait(barrier, len(peers))


def block_of(t):
    c, phase, unit, d, k = t
    n1, n2, _ = lens(c)
    return (c, d * k % n1, unit[0] % n2) if phase == 1 else (c, 0, d * k % n2 if phase == 2 else 0)


class Loads:
    def __init__(self, p, terms, T, sem):
        self.p, self.terms, self.T, self.sem = p, terms, T, sem
        self.left = list(dict.fromkeys([block_of(t) for t in REDUCE_ORDER] + [(c, 0, 0) for c in COLOURS]))
        self.place = {part: i % AHEAD for i, part in enumerate(self.left)}

    def at(self, part):
        c, k, o = part
        return self.p.off(DIMS[c][0], k), self.p.off(DIMS[c][1], o)

    def start(self, count):
        gate, up, down = self.terms
        for part in self.left[:count]:
            c, (i, j), s = part[0], self.at(part), self.sem.at[self.place[part]]
            T = self.T[c].at[i, j]
            if c == "A":
                for z in range(Z):
                    src = (gate, up)[z // X].at[z // 2 % 2, i, j, :, z % 2, pl.ds(0, LEFT)]
                    pltpu.make_async_copy(src, T.at[z], s).start()
            elif c == "B":
                pltpu.make_async_copy(down.at[lax.rem(j, 2), :, i, lax.div(j, 2)], T, s).start()
            else:
                layer, half = lax.rem(lax.div(i, 2), 2), lax.rem(i, 2)

                def load(ref):
                    pltpu.make_async_copy(ref.at[layer, j, :, :, half, pl.ds(LEFT, HALF - LEFT)], T, s).start()

                pl.when(i < X)(lambda: load(gate))
                pl.when(i >= X)(lambda: load(up))
        self.left = self.left[count:]

    def wait(self, part):
        if part in self.place:
            ref = self.T[part[0]].at[self.at(part)]
            pltpu.make_async_copy(ref, ref, self.sem.at[self.place.pop(part)]).wait()
            self.start(1)


class Reduce:
    def __init__(self, p, T, O, load, sent, arrived):
        self.p, self.T, self.O, self.load, self.sent, self.arrived = p, T, O, load, sent, arrived
        self.waited = set()


    def areas(self, t):
        c, phase, unit, d, k = t
        n1, n2, n3 = lens(c)
        d1, d2, d3 = DIMS[c]
        p = self.p
        slot = slots(SIZE[DIMS[c][phase - 1]], -ant_in(phase, unit))[d, k]
        if phase == 1:
            j2 = p.off(d2, unit[0])
            first, count = (0, n3) if unit[1] is None else (p.off(d3, unit[1]), 1)
            return (p.off(d1, d * k), j2), first, (slot, j2), first, count
        if phase == 2:
            first, count = (0, n3) if unit[0] is None else (p.off(d3, unit[0]), 1)
            return (p.at[d1], p.off(d2, d * k)), first, (n1 - 1, slot), first, count
        return (p.at[d1], p.at[d2]), p.off(d3, d * k), (n1 - 1, n2 - 1), slot, 1

    def copy(self, t):
        c, phase, _, d, _ = t
        src, i, dst, j, n = self.areas(t)
        s = R_ID[t]
        return pltpu.make_async_remote_copy(
            src_ref=self.T[c].at[(*src, pl.ds(i, n))],
            dst_ref=self.O[c].at[(*dst, pl.ds(j, n))],
            send_sem=self.sent.at[S_ID[c, phase]],
            recv_sem=self.arrived.at[s],
            device_id=self.p.beside[DIMS[c][phase - 1], d],
            device_id_type=MESH,
        )

    def wait(self, t):
        if t not in self.waited:
            self.waited.add(t)
            self.copy(t).wait_recv()

    def ended(self, c, phase, j2, j3):
        last = lens(c)[0] - 1
        return [(0, j2, j3), (1, j2, j3), (last, 0, j3), (last, 1, j3)][: 2 * (phase - 1)]

    def send(self, t):
        c, phase, unit, d, k = t
        T, O = self.T[c], self.O[c]
        for w in REDUCE[t][2]:
            self.wait(w)
        self.load.wait(block_of(t))
        src, first, _, _, count = self.areas(t)
        before = (c, phase, unit, d, k + 1)
        chain = before in R_ID
        if phase > 1 or chain:
            _, _, there, start, _ = self.areas(before if chain else t)

            def one(i):
                parts = self.ended(c, phase, src[1], first + i)
                if chain:
                    parts.append((*there, start + i))
                total = T[(*src, first + i)].astype(F32)
                for part in parts:
                    total = total + O[part].astype(F32)
                T[(*src, first + i)] = total.astype(BF16)

            if count == 1:
                one(0)
            else:
                pl.loop(0, count)(one)
        self.copy(t).start()

    def own(self, c):
        n1, n2, _ = lens(c)
        for t in REDUCE:
            if t[0] == c and t[-1] == 1 and not any(t[2]):
                self.wait(t)
        self.load.wait((c, 0, 0))
        i, j, k = (self.p.at[d] for d in DIMS[c])
        total = self.T[c][i, j, k].astype(F32)
        for part in self.ended(c, 3, j, k) + [(n1 - 1, n2 - 1, e) for e in (0, 1)]:
            total = total + self.O[c][part].astype(F32)
        return total.astype(BF16).astype(F32)


class Gather:
    def __init__(self, p, O, sent, arrived):
        self.p, self.O, self.sent, self.arrived = p, O, sent, arrived
        self.waited = set()

    def copy(self, t, came=0):
        c, phase, unit, d, k = t
        d1, d2, d3 = DIMS[c]
        p, dim = self.p, DIMS[c][phase - 1]
        behind = p.off(dim, d * (1 - came - k))
        at = (behind, p.off(d2, unit[0])) if phase == 1 else (p.at[d1], behind) if phase == 2 else (p.at[d1], p.at[d2], behind)
        at += tuple(p.off(d3, o) for o in unit[-1:] if o is not None)
        ref, s = self.O[c].at[at], G_ID[t]
        return pltpu.make_async_remote_copy(
            src_ref=ref,
            dst_ref=ref,
            send_sem=self.sent.at[S_ID[c, phase]],
            recv_sem=self.arrived.at[s],
            device_id=p.beside[dim, d],
            device_id_type=MESH,
        )

    def wait(self, t):
        if t not in self.waited:
            self.waited.add(t)
            self.copy(t, 1).wait_recv()

    def send(self, t):
        for w in GATHER[t][2]:
            self.wait(w)
        self.copy(t).start()


def rows_of(a):
    return lax.broadcasted_iota(jnp.int32, a.shape, a.ndim - 2)


def joined(a, b, k):
    return pltpu.roll(jnp.where(rows_of(b) >= ROWS - k, a, b), k, b.ndim - 2)


def adamw(w, m, v, g):
    m = 0.9 * m + 0.1 * g
    v = 0.95 * v + 0.05 * g * g
    return w - 0.02 * (m * lax.rsqrt(v + 1e-8) + 0.1 * w), m, v


DOWN_ROWS = (ROWS, ROWS, ROWS // 2)
SCRATCH = {
    "raw": ((2, 2, HIGH, LAYERS, FF), F32),
    "raw_down": ((2, 20, LAYERS, D), F32),
    "own": ((HIGH, HALF, *TILE), F32),
    "own_low": ((PART, HIGH, *TILE), F32),
    "old": ((2, LAYERS, 2, 2, HALF, *TILE), BF16),
    "old_down": ((LAYERS, 3, HIGH, *TILE), BF16),
    "w": ((2, LAYERS, 2 * HALF, *TILE), F32),
    "w_low": ((LAYERS, 3, HIGH, *TILE), F32),
    "mv": ((2, 2, LAYERS, 2 * HALF, *TILE), F32),
    "mv_low": ((2, LAYERS, 3, HIGH, *TILE), F32),
    "out": ((Z, HALF, *TILE), BF16),
    "into": ((Z, HALF, *TILE), BF16),
    "out_low": ((2, 3, HIGH, *TILE), BF16),
    "into_low": ((LAYERS, 3, HIGH, *TILE), BF16),
    "new": ((Z, HALF, *TILE), BF16),
    "news": ((Z, HALF, *TILE), BF16),
    "new_low": ((LAYERS, 3, HIGH, *TILE), BF16),
    "news_low": ((2, 3, HIGH, *TILE), BF16),
    "z_sum": ((Z, 1, LANES), F32),
    "sum": ((X * Y, 1, LANES), F32),
}


class Few:
    def __init__(self, p, sent, arrived):
        self.p, self.sent, self.arrived, self.waits = p, sent, arrived, []

    def exchange(self, copies, get):
        i = len(self.waits)
        for src, dst, to in copies:
            one = pltpu.make_async_remote_copy(
                src_ref=src, dst_ref=dst, send_sem=self.sent.at[i], recv_sem=self.arrived.at[i], device_id=to, device_id_type=MESH
            )
            one.start()
        self.waits.append(pltpu.make_async_copy(get, get, self.sent.at[i]).wait)
        return pltpu.make_async_copy(get, get, self.arrived.at[i]).wait

    def line(self, out, into, make):
        p, i = self.p, len(self.waits)
        z, get = p.at["z"], into.at[pl.ds(0, Z - 1)]
        for k in range(Z):
            make(k)

            @pl.when(z != k)
            def _():
                pltpu.make_async_remote_copy(
                    src_ref=out.at[k],
                    dst_ref=into.at[z],
                    send_sem=self.sent.at[i],
                    recv_sem=self.arrived.at[i],
                    device_id=p.device(z=k),
                    device_id_type=MESH,
                ).start()

        into[z] = out[z]
        self.waits.append(pltpu.make_async_copy(get, get, self.sent.at[i]).wait)
        return pltpu.make_async_copy(get, get, self.arrived.at[i]).wait

    def tell(self, ref, at, devices):
        return self.exchange([(ref.at[at], ref.at[at], to) for to in devices], ref.at[pl.ds(0, len(devices))])


def lanes(c):
    return pl.ds(pl.multiple_of(c * LANES, LANES), LANES)


def work(*refs):
    terms, weights, moments, refs = refs[:3], refs[3:6], refs[6:12], refs[12:]
    outs, made, refs = refs[:3], refs[3:9], refs[9:]
    O, T, refs = dict(zip(COLOURS, outs)), dict(zip(COLOURS, refs)), refs[3:]
    s = dict(zip(SCRATCH, refs))
    load, small, turn, sent, arrived, few_sent, few_arrived = refs[len(SCRATCH) :]
    p = Place()
    x, y, z = p.at.values()
    all_here = greet(p)
    loads = Loads(p, terms, T, load)
    loads.start(AHEAD)

    def rows_fetch():
        first = (X * Y * PART) * x + 20 * y + lax.div(PART * z, 2)
        for layer in range(LAYERS):
            for w in range(2):
                for i, row in enumerate((lax.max(z - 1, 0), lax.min(z, HIGH - 1))):
                    pltpu.make_async_copy(weights[w].at[layer, x, y, row], s["old"].at[w, layer, i], small.at[0]).start()
            pltpu.make_async_copy(weights[2].at[layer, pl.ds(first, 3)], s["old_down"].at[layer], small.at[1]).start()
        for i in range(2):
            for w in range(2):
                pltpu.make_async_copy(moments[3 * i + w], s["raw"].at[i, w], small.at[2]).start()
            pltpu.make_async_copy(moments[3 * i + 2], s["raw_down"].at[i], small.at[3]).start()

    def rows_here():
        for i, name in enumerate(("old", "old_down", "raw", "raw_down")):
            pltpu.make_async_copy(s[name], s[name], small.at[i]).wait()

    chores, later = [rows_fetch, rows_here], []

    def rows_in(w, layer):
        low, high = (s["old"][w, layer, i].reshape(2 * HALF, *TILE).astype(F32) for i in range(2))
        s["w"][w, layer] = joined(low, high, z)

    def rows_in_low(layer):
        part = [s["old_down"][layer, j].astype(F32) for j in range(3)]
        for j in range(3):
            s["w_low"][layer, j] = jnp.where(lax.rem(z, 2) == 1, joined(part[j], part[min(j + 1, 2)], ROWS // 2), part[j])

    def moments_in(i, w, layer):
        @pl.loop(0, 2 * HALF)
        def _(c):
            s["mv"][i, w, layer, c, pl.ds(0, HIGH)] = s["raw"][i, w, :, layer, lanes(c)]

    def moments_in_low(i, layer):
        @pl.loop(0, HIGH)
        def _(c):
            for j, n in enumerate(DOWN_ROWS):
                s["mv_low"][i, layer, j, c, pl.ds(0, n)] = s["raw_down"][i, pl.ds(ROWS * j, n), layer, lanes(c)]

    def moments_out(i, w, layer):
        @pl.loop(0, 2 * HALF)
        def _(c):
            rows = pl.ds(LAYERS * c + layer, HIGH, stride=LAYERS * 2 * HALF)
            made[3 * i + w][rows, :] = s["mv"][i, w, layer, c, pl.ds(0, HIGH)]

    def moments_out_low(i, layer):
        @pl.loop(0, HIGH)
        def _(c):
            for j, k in enumerate(DOWN_ROWS):
                rows = pl.ds(ROWS * j * LAYERS * HIGH + LAYERS * c + layer, k, stride=LAYERS * HIGH)
                made[3 * i + 2][rows, :] = s["mv_low"][i, layer, j, c, pl.ds(0, k)]

    for layer in range(LAYERS):
        for w in range(2):
            chores.append(functools.partial(rows_in, w, layer))
            for i in range(2):
                chores.append(functools.partial(moments_in, i, w, layer))
                later.append(functools.partial(moments_out, i, w, layer))
        chores.append(functools.partial(rows_in_low, layer))
        for i in range(2):
            chores.append(functools.partial(moments_in_low, i, layer))
            later.append(functools.partial(moments_out_low, i, layer))

    all_here()
    reduce = Reduce(p, T, O, loads, sent, arrived)
    pl.when(p.rep == 0)(lambda: pl.semaphore_wait(turn, 1))
    for n, t in enumerate(REDUCE_ORDER):
        reduce.send(t)
        if n == TURN:
            pl.when(p.rep == 1)(lambda: pl.semaphore_signal(turn, inc=1, device_id=p.twin, device_id_type=MESH))
        if n > len(REDUCE_ORDER) // 4 and n % 4 == 0 and chores:
            chores.pop(0)()

    few = Few(p, few_sent, few_arrived)
    squares = jnp.zeros(TILE, F32)
    for c in COLOURS:
        g = reduce.own(c)
        if c == "B":
            s["own_low"][...] = g
        else:
            s["own"][:, pl.ds(*((0, LEFT) if c == "A" else (LEFT, HALF - LEFT)))] = g
        squares = squares + jnp.sum((g * g).reshape(tiles(c), *TILE), axis=0)
    s["z_sum"][z] = jnp.sum(squares, axis=0, keepdims=True)
    line_sums = few.tell(s["z_sum"], z, p.line_device[1:])

    def piece(k):
        at = s["own"][min(k, HIGH - 1)]
        s["out"][k] = (joined(s["own"][k - 1], at, k) if k else at).astype(BF16)

    pieces = few.line(s["out"], s["into"], piece)
    g = [s["own_low"][j] for j in range(PART)]
    for j in range(3):
        s["out_low"][0, j] = g[j].astype(BF16)
        s["out_low"][1, j] = joined(g[2 + j], g[min(3 + j, PART - 1)], ROWS // 2).astype(BF16)
    mine = lax.rem(z, 2)
    other, partner = 1 - mine, p.device(z=z + 1 - 2 * mine)
    pieces_low = few.exchange([(s["out_low"].at[other], s["into_low"].at[mine], partner)], s["into_low"].at[other])
    s["into_low"][mine] = s["out_low"][mine]

    line_sums()
    at = Y * x + y
    s["sum"][at] = jnp.sum(s["z_sum"][...], axis=0)
    sums = few.tell(s["sum"], at, p.plane_device[1:])
    pieces()
    pieces_low()
    sums()
    total = jnp.sum(jnp.sum(s["sum"][...], axis=0), axis=1, keepdims=True)
    factor = jnp.minimum(1.0, 0.5 * lax.rsqrt(total / COUNT + 1e-30))

    def step(owner):
        w, layer, part = owner // X, owner // 2 % 2, pl.ds(owner % 2 * HALF, HALF)
        g = s["into"][owner].astype(F32) * factor
        new, m, v = adamw(s["w"][w, layer, part], s["mv"][0, w, layer, part], s["mv"][1, w, layer, part], g)
        s["mv"][0, w, layer, part], s["mv"][1, w, layer, part] = m, v
        s["new"][owner] = new.astype(BF16)

    pieces = few.line(s["new"], s["news"], step)
    for layer in range(LAYERS):
        g = s["into_low"][layer].astype(F32) * factor
        new, m, v = adamw(s["w_low"][layer], s["mv_low"][0, layer], s["mv_low"][1, layer], g)
        s["mv_low"][0, layer], s["mv_low"][1, layer] = m, v
        s["new_low"][layer] = new.astype(BF16)
    pieces_low = few.exchange([(s["new_low"].at[other], s["news_low"].at[mine], partner)], s["news_low"].at[other])
    s["news_low"][mine] = s["new_low"][mine]

    own = {c: tuple(p.at[d] for d in DIMS[c]) for c in COLOURS}

    def whole_low():
        pieces_low()
        a, b = ([s["news_low"][i, j].astype(F32) for j in range(3)] for i in range(2))
        seam = jnp.where(rows_of(b[0]) < ROWS // 2, a[2], pltpu.roll(b[0], ROWS // 2, 1))
        for i, tile in enumerate((a[0], a[1], seam, *(joined(b[j], b[j + 1], ROWS // 2) for j in range(2)))):
            O["B"][(*own["B"], i)] = tile.astype(BF16)

    def whole():
        pieces()
        t = [s["news"][k].astype(F32) for k in range(Z)]
        for i in range(HIGH):
            a = pltpu.roll(t[i], ROWS - i, 1) if i else t[i]
            tile = jnp.where(rows_of(a) < HIGH - i, a, pltpu.roll(t[i + 1], HIGH - i, 1)).astype(BF16)
            O["A"][(*own["A"], i)] = tile[:LEFT]
            O["C"][(*own["C"], i)] = tile[LEFT:]

    all_sent(T, sent)
    gather = Gather(p, O, sent, arrived)
    prepare = {"B": whole_low, "A": whole}
    for n, t in enumerate(GATHER_ORDER):
        needs = "B" if t[0] == "B" else "A"
        if needs in prepare:
            prepare.pop(needs)()
        gather.send(t)
        if n > len(GATHER_ORDER) // 4 and n % 4 == 0 and later:
            later.pop(0)()
    for t in GATHER_ENDS:
        gather.wait(t)
    for wait in few.waits:
        wait()
    all_sent(T, sent)


def put(*refs):
    (a, b, c), moments, results, sem = refs[:3], refs[3:9], refs[9:18], refs[18]

    def copy(src, i, *at):
        pltpu.make_async_copy(src, results[i].at[at] if at else results[i], sem.at[i]).start()

    for z in range(Z):
        half, layer = z % 2, z // 2 % 2
        copy(a.at[:, :, z], z // X, layer, slice(None), slice(None), slice(None), half, pl.ds(0, LEFT))
        copy(c.at[z], z // X, layer, slice(None), slice(None), slice(None), half, pl.ds(LEFT, HALF - LEFT))
        layer, q = down_place(z)
        for y in range(Y):
            copy(b.at[y, z], 2, layer, slice(None), y, q)
    for i, moment in enumerate(moments):
        copy(moment, 3 + i)
    for i, ref in enumerate(results):
        pltpu.make_async_copy(ref, ref, sem.at[i]).wait()


def tiled(a, *cut):
    rows, columns = cut
    n = len(rows)
    a = a.reshape(LAYERS, *rows, ROWS, *columns, LANES)
    order = [*range(n + 1), *range(n + 2, n + 2 + len(columns)), n + 1, a.ndim - 1]
    return a.transpose(order)


def untiled(a, *cut):
    rows, columns = cut
    n = len(rows)
    order = [*range(n + 1), a.ndim - 2, *range(n + 1, a.ndim - 2), a.ndim - 1]
    a = a.transpose(order)
    return a.reshape(LAYERS, -1, a.shape[-1] * (HALF * 2 if len(columns) == 2 else HIGH))


WIDE, TALL = ((X, Y, HIGH), (2, HALF)), ((X, Y, X, PART), (HIGH,))


def unmoment(a, rows, columns):
    return a.reshape(rows, columns, LAYERS, LANES).transpose(0, 2, 1, 3).reshape(rows, LAYERS, columns * LANES).transpose(1, 0, 2)


def solution(mesh):
    shapes = [pltpu.VMEM((*lens(c), *BLOCK[c], *TILE), BF16) for c in COLOURS]
    hbm, vmem = pl.BlockSpec(memory_space=pltpu.HBM), pl.BlockSpec(memory_space=pltpu.VMEM)
    moment = (LAYERS * HIGH * HALF * 2, LANES)

    def semaphores(n):
        return pltpu.SemaphoreType.DMA((n,))

    def kernel(body, name, params, **more):
        return pl.pallas_call(body, name=name, compiler_params=pltpu.CompilerParams(**params), **more)

    def step(*arrays):
        terms, weights, moments = [t[0] for t in arrays[:3]], arrays[3:6], arrays[6:]
        wide = [tiled(a, *WIDE) for a in (*terms[:2], *weights[:2])]
        operands = [*wide[:2], tiled(terms[2], *TALL), *wide[2:], tiled(weights[2], (FF // ROWS,), (HIGH,))]
        operands += [a.transpose(1, 0, 2) for a in moments]
        made = kernel(
            work,
            "work",
            dict(collective_id=0, has_side_effects=True, vmem_limit_bytes=34 << 20),
            out_shape=(*shapes, *[pltpu.VMEM(moment, F32)] * 6),
            in_specs=[hbm] * 12,
            out_specs=[vmem] * 9,
            scratch_shapes=[
                *shapes,
                *(pltpu.VMEM(*a) for a in SCRATCH.values()),
                semaphores(AHEAD),
                semaphores(4),
                pltpu.SemaphoreType.REGULAR,
                *(semaphores(n) for n in (len(S_ID), len(R_ID), 6, 6)),
            ],
        )(*(pltpu.with_memory_space_constraint(a, pltpu.HBM) for a in operands))
        out = kernel(
            put,
            "put",
            dict(vmem_limit_bytes=1 << 20),
            out_shape=[jax.ShapeDtypeStruct(a.shape, BF16) for a in operands[:3]] + [jax.ShapeDtypeStruct(moment, F32)] * 6,
            in_specs=[vmem] * 9,
            out_specs=[hbm] * 9,
            scratch_shapes=[semaphores(9)],
        )(*made)
        weights = [untiled(a, *cut) for a, cut in zip(out, (WIDE, WIDE, TALL))]
        return (*weights, *(unmoment(a, *m.shape[1:2], m.shape[2] // LANES) for a, m in zip(out[3:], moments)))

    all_of, cut = P(None, None, None), P(None, "dp", None)
    return jax.shard_map(
        step,
        mesh=mesh,
        in_specs=(P(("rep", "dp"), None, None, None),) * 3 + (all_of,) * 3 + (cut,) * 6,
        out_specs=(P("rep", None, None),) * 3 + (P("rep", "dp", None),) * 6,
        check_vma=False,
    )
```
